128 devices in a mesh: group: 4 (over z), sub: 32 (over y, x, core).
Axes of the slice: x: 4, y: 4, z: 4, core: 2. Of those that a mesh axis runs over, the one named last changes fastest.
Arguments:
- displacement: float32 [3, 35, 131072], P(None, None, ('group', 'sub')), may hold values from -6 to 6
- velocity: float32 [3, 35, 131072], P(None, None, ('group', 'sub')), may hold values from -6 to 6
- geometry_weights: float32 [6, 131072], P(None, ('group', 'sub')), may hold values from 0.2 to 2
- jacobian: float32 [131072], P(('group', 'sub')), may hold values from 0.5 to 2
- strain_map: float32 [630, 105], replicated, may hold values from -0.25 to 0.25
- face_mass: float32 [15, 15], replicated, may hold values from -1 to 2, as said below
- mass_inverse: float32 [35, 35], replicated, may hold values from -1 to 2, as said below
- local_links: int32 [2, 393216], P(None, ('group', 'sub')), may hold values from 0 to 383, as said below
- local_geometry: float32 [4, 393216], P(None, ('group', 'sub')), may hold values from -1 to 3, as said below
- neighbour_links: int32 [2, 16384], P(None, ('group', 'sub')), may hold values from 0 to 2, as said below
- neighbour_geometry: float32 [8, 16384], P(None, ('group', 'sub')), may hold values from -1 to 3, as said below
- cross_links: int32 [98304], P(('group', 'sub')), may hold values from 0 to 2, as said below
- cross_geometry: float32 [4, 98304], P(None, ('group', 'sub')), may hold values from -1 to 3, as said below
Outputs:
- displacement_new: float32 [3, 35, 131072], P(None, None, ('group', 'sub'))
- velocity_new: float32 [3, 35, 131072], P(None, None, ('group', 'sub'))
The draws below stay inside these ranges and needn't reach their ends.
Inputs may be any that keep to these rules, and one draw needn't show every extreme that they name: `local_links`: row 0 is the partner inside the same aligned block of 128 elements, as the steps read it; the pairing is symmetric and never pairs a half-face with itself. Row 1 is the state (0 intact, 1 cohesive, 2 broken), equal on both half-faces of a pair. `local_geometry`: rows 0 to 2 are a unit normal, row 3 a positive scale; both half-faces of a pair hold the same values. `neighbour_links`: row 0: state of the upper shared half-face, row 1: of the lower one (0 intact, 1 cohesive, 2 broken). Row 1 of device (g, s) equals row 0 of the same column on device (g, (s - 1) mod 32). `neighbour_geometry`: rows 0 to 3: unit normal and positive scale of the upper half-face; rows 4 to 7 of device (g, s) equal rows 0 to 3 of the same column on device (g, (s - 1) mod 32). `cross_links`: states (0 intact, 1 cohesive, 2 broken). In the block of 8 slots that a device holds for one partner device, the first count slots hold faces and the rest are padding with state 2; count is the same on both sides of a pair, 1 to 8, 8 for some pair, and the states of matching slots agree. `cross_geometry`: rows 0 to 2 a unit normal, row 3 a positive scale; matching slots of a pair hold the same values. `face_mass`: Symmetric. `mass_inverse`: Symmetric.
All inputs are finite; a program needn't handle non-finite values.
Results may differ from the reference program's by a relative error of at most 0.00011.
Values sent between devices are 32-bit elements; how exact they have to be, the bound alone decides.
A program may use at most 128 MiB of HBM per device.

```python
import math
import jax
import jax.numpy as jnp
import numpy as np
from jax import lax

COMP = 3
NODES = 35
FNODES = 15
NMAT = 6
SLOT = 8
BLOCK = 128
STEPS = 5
E_DEV = 1024
ELEMS = 131072
F_NB = 128
CROSS = 768
N_GROUP = 4
N_SUB = 32
DEVICES = 128


def face_states(key, shape):
    level = jax.random.randint(key, shape, 0, 8)
    return jnp.where(level < 5, 0, jnp.where(level < 7, 1, 2)).astype(jnp.int32)


def face_geometry(key, count):
    first, second, third = jax.random.split(key, 3)
    height = jax.random.uniform(first, (count,), jnp.float32, -1.0, 1.0)
    azimuth = jax.random.uniform(second, (count,), jnp.float32, -math.pi, math.pi)
    radial = jnp.sqrt(jnp.maximum(1.0 - height * height, 0.0))
    scale = jnp.exp(jax.random.uniform(third, (count,), jnp.float32, math.log(0.3), math.log(3.0)))
    return jnp.stack([radial * jnp.cos(azimuth), radial * jnp.sin(azimuth), height, scale])


def definite(key, order):
    first, second = jax.random.split(key)
    diagonal = jax.random.uniform(first, (order,), jnp.float32, 0.8, 1.2)
    spread = 0.75 / order
    offside = jax.random.uniform(second, (order, order), jnp.float32, -spread, spread)
    offside = 0.5 * (offside + offside.T)
    offside = offside * (1.0 - jnp.eye(order, dtype=jnp.float32))
    return offside + jnp.diag(diagonal)


def draw_face_mass(key, part):
    return definite(jax.random.fold_in(key, 3), FNODES)


def draw_mass_inverse(key, part):
    return definite(jax.random.fold_in(key, 5), NODES)


def local_pairing(key):
    blocks = DEVICES * (E_DEV // BLOCK)
    width = 3 * BLOCK
    scores = jax.random.randint(key, (blocks, width), 0, 1 << 20) * width + jnp.arange(width, dtype=jnp.int32)[None, :]
    order = jnp.argsort(scores, axis=1).astype(jnp.int32)
    swapped = order.reshape(blocks, width // 2, 2)[:, :, ::-1].reshape(blocks, width)
    rows = jnp.arange(blocks, dtype=jnp.int32)[:, None]
    partner = jnp.zeros((blocks, width), jnp.int32).at[rows, order].set(swapped)
    labels = jnp.broadcast_to(jnp.repeat(jnp.arange(width // 2, dtype=jnp.int32), 2)[None, :], (blocks, width))
    pair_index = jnp.zeros((blocks, width), jnp.int32).at[rows, order].set(labels)
    return (partner, pair_index)


def to_columns(blocked):
    leading = blocked.shape[0]
    shaped = blocked.reshape(leading, DEVICES, E_DEV // BLOCK, 3, BLOCK)
    return jnp.transpose(shaped, (0, 1, 3, 2, 4)).reshape(leading, 3 * E_DEV * DEVICES)


def draw_local_links(key, part):
    partner, pair_index = local_pairing(jax.random.fold_in(key, 11))
    blocks = partner.shape[0]
    pair_states = face_states(jax.random.fold_in(key, 12), (blocks, 3 * BLOCK // 2))
    states = jnp.take_along_axis(pair_states, pair_index, axis=1)
    return to_columns(jnp.stack([partner, states])).astype(jnp.int32)


def draw_local_geometry(key, part):
    partner, pair_index = local_pairing(jax.random.fold_in(key, 11))
    blocks = partner.shape[0]
    drawn = face_geometry(jax.random.fold_in(key, 13), blocks * (3 * BLOCK // 2)).reshape(4, blocks, 3 * BLOCK // 2)
    spread = jnp.take_along_axis(drawn, jnp.broadcast_to(pair_index[None], (4, blocks, 3 * BLOCK)), axis=2)
    return to_columns(spread)


def draw_neighbour_links(key, part):
    count = F_NB * DEVICES
    upper_state = face_states(jax.random.fold_in(key, 17), (count,))
    lower_state = jnp.roll(upper_state.reshape(N_GROUP, N_SUB, F_NB), 1, axis=1).reshape(count)
    return jnp.stack([upper_state, lower_state]).astype(jnp.int32)


def draw_neighbour_geometry(key, part):
    count = F_NB * DEVICES
    upper = face_geometry(jax.random.fold_in(key, 19), count)
    lower = jnp.roll(upper.reshape(4, N_GROUP, N_SUB, F_NB), 1, axis=2).reshape(4, count)
    return jnp.concatenate([upper, lower], axis=0)


def to_layout(dense):
    ranks = jnp.arange(DEVICES, dtype=jnp.int32)
    offsets = jnp.arange(N_GROUP - 1, dtype=jnp.int32)
    places = jnp.arange(N_SUB, dtype=jnp.int32)
    groups = ranks // N_SUB
    partners = (groups[:, None, None] + 1 + offsets[None, :, None]) % N_GROUP * N_SUB + places[None, None, :]
    partners = partners.reshape(DEVICES, (N_GROUP - 1) * N_SUB)
    picked = dense[:, ranks[:, None], partners]
    return picked.reshape(dense.shape[0], DEVICES * CROSS)


def draw_cross_links(key, part):
    devices = DEVICES
    keys = jax.random.split(jax.random.fold_in(key, 23), 3)
    lowest = max(1, 3 * SLOT // 8)
    base = jax.random.randint(keys[0], (devices, devices), lowest, SLOT + 1)
    busy = jax.random.randint(keys[1], (devices,), 0, 4) == 0
    counts = jnp.where(busy[:, None] | busy[None, :], base, (base + 1) // 2)
    ranks = jnp.arange(devices, dtype=jnp.int32)
    lower_rank = ranks[:, None] < ranks[None, :]
    counts = jnp.where(lower_rank, counts, counts.T)
    filled = (ranks[:, None] == 0) & (ranks[None, :] == N_SUB) | (ranks[:, None] == N_SUB) & (ranks[None, :] == 0)
    counts = jnp.where(filled, SLOT, counts)
    states = face_states(keys[2], (devices, devices, SLOT))
    states = jnp.where(lower_rank[:, :, None], states, jnp.transpose(states, (1, 0, 2)))
    used = jnp.arange(SLOT, dtype=jnp.int32)[None, None, :] < counts[:, :, None]
    stacked = jnp.where(used, states, 2)[None]
    return to_layout(stacked).reshape(DEVICES * CROSS).astype(jnp.int32)


def draw_cross_geometry(key, part):
    devices = DEVICES
    drawn = face_geometry(jax.random.fold_in(key, 29), devices * devices * SLOT).reshape(4, devices, devices, SLOT)
    ranks = jnp.arange(devices, dtype=jnp.int32)
    lower_rank = (ranks[:, None] < ranks[None, :])[None, :, :, None]
    drawn = jnp.where(lower_rank, drawn, jnp.transpose(drawn, (0, 2, 1, 3)))
    return to_layout(drawn)


def shard_levels(key, dims, cuts, low, high):
    level = 1.0
    for axis_at, shards_of in cuts:
        steps = jax.random.uniform(jax.random.fold_in(jax.random.fold_in(key, 6), axis_at), (shards_of,), jnp.float32, low / len(cuts), high / len(cuts))
        level = level * jnp.repeat(jnp.exp(steps), dims[axis_at] // shards_of).reshape((-1,) + (1,) * (len(dims) - 1 - axis_at))
    return level


def centred(own_key, shape, scale, bound, shards=(), kind=jnp.bfloat16):
    gain = shard_levels(own_key, shape, shards, -0.22, 0.18) if shards else 1.0
    values = jax.random.normal(own_key, shape, jnp.float32) * scale * gain
    return jnp.minimum(jnp.maximum(values, -bound), bound).astype(kind)


def setup_inputs(seed: int = 0) -> dict:
    key_of = jax.random.split(jax.random.key(seed), 14)
    return {
        "displacement": centred(key_of[0], (COMP, NODES, ELEMS), 1.0, 6.0, ((2, 128),), jnp.float32),
        "velocity": centred(key_of[1], (COMP, NODES, ELEMS), 1.0, 6.0, ((2, 128),), jnp.float32),
        "geometry_weights": jnp.clip(jnp.exp(math.log(2.0) - 2.3025851 * jax.random.uniform(key_of[2], (NMAT, ELEMS), jnp.float32) ** shard_levels(key_of[2], (NMAT, ELEMS), ((1, 128),), -0.2, 0.2)), 0.2, 2.0),
        "jacobian": jnp.clip(jnp.exp(math.log(2.0) - 1.3862944 * jax.random.uniform(key_of[3], (ELEMS,), jnp.float32) ** shard_levels(key_of[3], (ELEMS,), ((0, 128),), -0.2, 0.2)), 0.5, 2.0),
        "strain_map": centred(key_of[4], (NMAT * COMP * NODES, COMP * NODES), (NMAT * COMP * NODES) ** -0.5, 0.25, (), jnp.float32),
        "face_mass": draw_face_mass(jax.random.fold_in(key_of[13], 71), 0),
        "mass_inverse": draw_mass_inverse(jax.random.fold_in(key_of[13], 71), 0),
        "local_links": draw_local_links(jax.random.fold_in(key_of[13], 71), 0),
        "local_geometry": draw_local_geometry(jax.random.fold_in(key_of[13], 71), 0),
        "neighbour_links": draw_neighbour_links(jax.random.fold_in(key_of[13], 71), 0),
        "neighbour_geometry": draw_neighbour_geometry(jax.random.fold_in(key_of[13], 71), 0),
        "cross_links": draw_cross_links(jax.random.fold_in(key_of[13], 71), 0),
        "cross_geometry": draw_cross_geometry(jax.random.fold_in(key_of[13], 71), 0),
    }


shear_weight = 0.5
opening_scale = 4.0
time_step = 0.25
highest = lax.Precision.HIGHEST


def face_table():
    points = [(first, second, third, 4 - first - second - third) for first in range(5) for second in range(5 - first) for third in range(5 - first - second)]
    result = np.zeros((4, 15, 35), np.float32)
    for side in range(4):
        members = [index for index, point in enumerate(points) if point[side] == 0]
        for place, index in enumerate(members):
            result[side, place, index] = 1.0
    return result


def cohesive_traction(jump, normal, state):
    along = jnp.sum(normal[:, None, :] * jump, axis=0)
    normal_part = along[None] * normal[:, None, :]
    tangent = jump - normal_part
    opening = along * along + shear_weight * jnp.sum(tangent * tangent, axis=0)
    softened = jnp.exp(-opening / opening_scale)[None] * (normal_part + shear_weight * tangent)
    zeros = jnp.zeros_like(jump)
    return jnp.where(state[None, None, :] == 0, jump, jnp.where(state[None, None, :] == 1, softened, zeros))


def face_force(jump, geometry, state, face_mass):
    traction = cohesive_traction(jump, geometry[0:3], state)
    spread = jnp.einsum("ij,cjf->cif", face_mass, traction, precision=highest)
    return geometry[3][None, None, :] * spread


def flatten(array):
    return array.reshape(COMP, FNODES, -1)


def reference(displacement, velocity, geometry_weights, jacobian, strain_map, face_mass, mass_inverse, local_links, local_geometry, neighbour_links, neighbour_geometry, cross_links, cross_geometry):
    table = jnp.asarray(face_table())
    count_blocks = E_DEV // BLOCK
    partner = jnp.transpose(local_links[0].reshape(DEVICES, 3, count_blocks, BLOCK), (0, 2, 1, 3)).reshape(DEVICES * count_blocks, 3 * BLOCK)
    partner = jnp.broadcast_to(partner[None, None], (COMP, FNODES, DEVICES * count_blocks, 3 * BLOCK)).astype(jnp.int32)
    groups_at = jnp.arange(N_GROUP, dtype=jnp.int32)[:, None, None, None]
    places_at = jnp.arange(N_SUB, dtype=jnp.int32)[None, :, None, None]
    offsets_at = jnp.arange(N_GROUP - 1, dtype=jnp.int32)[None, None, :, None]
    targets_at = jnp.arange(N_SUB, dtype=jnp.int32)[None, None, None, :]
    other_group = (groups_at + 1 + offsets_at) % N_GROUP
    other_block = N_GROUP - 2 - offsets_at
    spare = E_DEV - 2 * F_NB - CROSS
    field = displacement
    for step in range(STEPS):
        traces = jnp.einsum("kin,cne->cike", table, field, precision=highest)
        own_local = jnp.transpose(traces[:, :, 1:].reshape(COMP, FNODES, 3, DEVICES, E_DEV), (0, 1, 3, 2, 4))
        blocked = jnp.transpose(own_local.reshape(COMP, FNODES, DEVICES, 3, count_blocks, BLOCK), (0, 1, 2, 4, 3, 5)).reshape(COMP, FNODES, DEVICES * count_blocks, 3 * BLOCK)
        paired = jnp.take_along_axis(blocked, partner, axis=3)
        paired = jnp.transpose(paired.reshape(COMP, FNODES, DEVICES, count_blocks, 3, BLOCK), (0, 1, 2, 4, 3, 5)).reshape(COMP, FNODES, DEVICES * 3 * E_DEV)
        local_force = face_force(paired - own_local.reshape(COMP, FNODES, DEVICES * 3 * E_DEV), local_geometry, local_links[1], face_mass)
        local_force = jnp.transpose(local_force.reshape(COMP, FNODES, DEVICES, 3, E_DEV), (0, 1, 3, 2, 4)).reshape(COMP, FNODES, 3, ELEMS)
        rim = traces[:, :, 0].reshape(COMP, FNODES, N_GROUP, N_SUB, E_DEV)
        upper = rim[..., 0:F_NB]
        lower = rim[..., F_NB:2 * F_NB]
        crossing = rim[..., 2 * F_NB:2 * F_NB + CROSS].reshape(COMP, FNODES, N_GROUP, N_SUB, N_GROUP - 1, N_SUB, SLOT)
        upper_force = face_force(flatten(jnp.roll(lower, -1, axis=3) - upper), neighbour_geometry[0:4], neighbour_links[0], face_mass)
        lower_force = face_force(flatten(jnp.roll(upper, 1, axis=3) - lower), neighbour_geometry[4:8], neighbour_links[1], face_mass)
        facing = crossing[:, :, other_group, targets_at, other_block, places_at, :]
        cross_force = face_force(flatten(facing - crossing), cross_geometry, cross_links, face_mass)
        shape = (COMP, FNODES, N_GROUP, N_SUB, -1)
        filler = jnp.zeros((COMP, FNODES, N_GROUP, N_SUB, spare), field.dtype)
        rim_force = jnp.concatenate([upper_force.reshape(shape), lower_force.reshape(shape), cross_force.reshape(shape), filler], axis=4).reshape(COMP, FNODES, ELEMS)
        forces = jnp.concatenate([rim_force[:, :, None], local_force], axis=2)
        face_load = jnp.einsum("kin,cike->cne", table, forces, precision=highest)
        strain = jnp.dot(strain_map, field.reshape(COMP * NODES, ELEMS), precision=highest)
        weighted = (strain.reshape(NMAT, COMP * NODES, ELEMS) * geometry_weights[:, None, :]).reshape(NMAT * COMP * NODES, ELEMS)
        volume = -jnp.dot(strain_map.T, weighted, precision=highest).reshape(COMP, NODES, ELEMS)
        acceleration = jnp.einsum("nm,cme->cne", mass_inverse, volume + face_load, precision=highest) / jacobian[None, None, :]
        velocity = velocity + time_step * acceleration
        field = field + time_step * velocity
    return field, velocity
```

```python
import functools

import jax
import jax.numpy as jnp
import numpy as np
from jax import lax
from jax.experimental import pallas as pl
from jax.experimental.pallas import tpu as pltpu
from jax.sharding import PartitionSpec as P

MESH = pl.DeviceIdType.MESH
HIGHEST = lax.Precision.HIGHEST
F32 = jnp.float32
BF16 = jnp.bfloat16

DT = 0.25
NODES = 35
FN = 15
LANES = 128
ROWS = 112
RIM = 48
REST = NODES - FN
PIECES = 6
GROUPS = 4
SUBS = 32
SLOT = 8
ROUNDS = 3


def row_of(c, n):
    return 16 * c + n if n < FN else RIM + REST * c + n - FN


def tables():
    points = [(a, b, c, 4 - a - b - c) for a in range(5) for b in range(5 - a) for c in range(5 - a - b)]
    faces = [[i for i, p in enumerate(points) if p[k] == 0] for k in range(4)]
    spread = np.zeros((ROWS, NODES), np.float32)
    perm = np.zeros((3 * NODES, ROWS), np.float32)
    select = np.zeros((4 * RIM, ROWS), np.float32)
    place = np.zeros((FN, 4 * RIM), np.float32)
    comp = np.full((ROWS,), -1, np.int64)
    for c in range(3):
        for n in range(NODES):
            spread[row_of(c, n), n] = 1.0
            perm[c * NODES + n, row_of(c, n)] = 1.0
            comp[row_of(c, n)] = c
        for k in range(4):
            for i, n in enumerate(faces[k]):
                select[k * RIM + 16 * c + i, row_of(c, n)] = 1.0
                place[i, k * RIM + 16 * c + i] = 1.0
    same = ((comp[:, None] == comp[None, :]) & (comp[:, None] >= 0)).astype(np.float32)
    block = np.arange(4 * RIM) // 16
    same_face = (block[:, None] == block[None, :]).astype(np.float32)
    return spread, perm, select, place, same, same_face


def dot(a, b, dims=((1,), (0,))):
    return lax.dot_general(a, b, (dims, ((), ())), precision=HIGHEST, preferred_element_type=F32)


def halves(x):
    high = x.astype(BF16)
    return high, (x - high.astype(F32)).astype(BF16)


def traction(j, u, rigid, soft):
    jn = u[0] * j[0] + u[1] * j[1] + u[2] * j[2]
    size = j[0] * j[0] + j[1] * j[1] + j[2] * j[2] + jn * jn
    e = soft * jnp.exp(size * -0.125)
    a = rigid + e
    b = e * jn
    return [a * j[c] + b * u[c] for c in range(3)]


def kernel(
    d_ref, v_ref, w_ref, jac_ref, s_ref, fm_ref, mi_ref, ll_ref, lg_ref, nl_ref, ng_ref, cl_ref, cg_ref,
    spread_ref, perm_ref, select_ref, place_ref, same_ref, face_ref,
    od_ref, ov_ref,
    f, v, fp, p, tp, amat, lmat, zmat, wj, ratio, lc, li, zc,
    xs, xr, ns, nr, xs_sem, xr_sem, ns_sem, nr_sem,
):
    g = lax.axis_index("group")
    s = lax.axis_index("sub")
    elements = f.shape[1]
    up = lax.rem(s + 1, SUBS)
    down = lax.rem(s + SUBS - 1, SUBS)
    barrier = pltpu.get_barrier_semaphore()

    def greet(t, carry):
        for b in range(GROUPS - 1):
            pl.semaphore_signal(
                barrier, inc=1, device_id=(lax.rem(g + 1 + b, GROUPS), t), device_id_type=MESH
            )
        return carry

    lax.fori_loop(0, SUBS, greet, 0)
    for t in (up, down):
        pl.semaphore_signal(barrier, inc=1, device_id=(g, t), device_id_type=MESH)

    jac = jac_ref[...].reshape(1, elements)
    inv = 1.0 / jac
    wj[...] = w_ref[...] * (inv * -DT)
    for q in range(3):
        part = pl.ds(q * elements, elements)
        state = ll_ref[1:2, part]
        scale = lg_ref[3:4, part] * (inv * DT)
        lc[q, 0:3, :] = lg_ref[0:3, part]
        lc[q, 3:4, :] = jnp.where(state == 0, scale, 0.0)
        lc[q, 4:5, :] = jnp.where(state == 1, 0.5 * scale, 0.0)
        partner = ll_ref[0:1, part]
        li[q, 0:1, :] = lax.rem(partner, LANES)
        li[q, 1:2, :] = lax.div(partner, LANES)
    cross = elements - 2 * LANES
    spots = (
        (0, LANES, ng_ref[0:4, :], nl_ref[0:1, :]),
        (LANES, LANES, ng_ref[4:8, :], nl_ref[1:2, :]),
        (2 * LANES, cross, cg_ref[...], cl_ref[...].reshape(1, cross)),
    )
    for at, size, geometry, state in spots:
        lanes = pl.ds(at, size)
        scale = geometry[3:4, :] * (inv[:, at : at + size] * DT)
        zc[0:3, lanes] = geometry[0:3, :]
        zc[3:4, lanes] = jnp.where(state == 0, scale, 0.0)
        zc[4:5, lanes] = jnp.where(state == 1, 0.5 * scale, 0.0)

    for source, target in ((d_ref, f), (v_ref, v)):
        for c in range(3):
            target[16 * c : 16 * c + FN, :] = source[c, 0:FN, :]
            target[16 * c + FN : 16 * c + FN + 1, :] = jnp.zeros((1, elements), F32)
            target[RIM + REST * c : RIM + REST * (c + 1), :] = source[c, FN:NODES, :]
        target[RIM + 3 * REST :, :] = jnp.zeros((ROWS - RIM - 3 * REST, elements), F32)
    f[FN : FN + 1, :] = inv

    spread = spread_ref[...]
    mass = dot(dot(spread, mi_ref[...]), spread, ((1,), (1,))) * same_ref[...]
    place = place_ref[...]
    face = dot(dot(place, fm_ref[...], ((0,), (0,))), place) * face_ref[...]
    lift = dot(mass, dot(select_ref[...], face, ((0,), (0,))))
    high, low = halves(lift)
    zmat[:, 0:RIM] = high[:, 0:RIM]
    zmat[:, RIM : 2 * RIM] = high[:, 0:RIM]
    zmat[:, 2 * RIM : 3 * RIM] = low[:, 0:RIM]
    lmat[:, 0 : 3 * RIM] = high[:, RIM:]
    lmat[:, 3 * RIM : 6 * RIM] = high[:, RIM:]
    lmat[:, 6 * RIM : 9 * RIM] = low[:, RIM:]
    for m in range(PIECES):
        piece = dot(s_ref[m * 3 * NODES : (m + 1) * 3 * NODES, :], perm_ref[...])
        high, low = halves(dot(mass, dot(piece, piece, ((0,), (0,)))))
        rows = slice(m * ROWS, (m + 1) * ROWS)
        amat[rows, 0:ROWS] = high
        amat[rows, ROWS : 2 * ROWS] = high
        amat[rows, 2 * ROWS : 3 * ROWS] = low
    chosen = select_ref[RIM:, :].astype(BF16)
    rows = slice(PIECES * ROWS, PIECES * ROWS + 3 * RIM)
    amat[rows, 0:ROWS] = chosen
    amat[rows, ROWS : 2 * ROWS] = chosen
    amat[rows, 2 * ROWS : 3 * ROWS] = jnp.zeros((3 * RIM, ROWS), BF16)

    def local(width=2 * LANES):
        for at in range(0, elements, width):
            lanes = pl.ds(at, width)
            old = f[:, lanes]
            high, low = halves(old)
            product = jnp.dot(
                amat[...], jnp.concatenate([high, low, high], axis=0), preferred_element_type=F32
            )
            change = wj[0:1, lanes] * product[0:ROWS, :]
            for m in range(1, PIECES):
                change = change + wj[m : m + 1, lanes] * product[m * ROWS : (m + 1) * ROWS, :]
            highs, lows = [], []
            trace = [product[PIECES * ROWS + q * RIM : PIECES * ROWS + (q + 1) * RIM, :] for q in range(3)]
            for q in range(3):
                pulls = []
                for block in range(0, width, LANES):
                    here = slice(block, block + LANES)
                    index = jnp.broadcast_to(li[q, 0:1, pl.ds(at + block, LANES)], (RIM, LANES))
                    origin = jnp.broadcast_to(li[q, 1:2, pl.ds(at + block, LANES)], (RIM, LANES))
                    found = [
                        jnp.take_along_axis(trace[r][:, here], index, axis=1, mode="promise_in_bounds")
                        for r in range(3)
                    ]
                    paired = jnp.where(origin == 0, found[0], jnp.where(origin == 1, found[1], found[2]))
                    jump = paired - trace[q][:, here]
                    at_lanes = pl.ds(at + block, LANES)
                    pulls.append(
                        jnp.concatenate(
                            traction(
                                [jump[16 * c : 16 * (c + 1), :] for c in range(3)],
                                [lc[q, c : c + 1, at_lanes] for c in range(3)],
                                lc[q, 3:4, at_lanes],
                                lc[q, 4:5, at_lanes],
                            ),
                            axis=0,
                        )
                    )
                high, low = halves(jnp.concatenate(pulls, axis=1))
                highs.append(high)
                lows.append(low)
            change = change + jnp.dot(
                lmat[...], jnp.concatenate(highs + lows + highs, axis=0), preferred_element_type=F32
            )
            speed = v[:, lanes] + change
            v[:, lanes] = speed
            fp[:, lanes] = old + DT * speed

    def rim(advance, width=2 * LANES):
        for at in range(0, elements, width):
            lanes = pl.ds(at, width)
            jump = p[:, lanes] - f[0:RIM, lanes]
            pull = jnp.concatenate(
                traction(
                    [jump[16 * c : 16 * (c + 1), :] for c in range(3)],
                    [zc[c : c + 1, lanes] for c in range(3)],
                    zc[3:4, lanes],
                    zc[4:5, lanes],
                ),
                axis=0,
            )
            high, low = halves(pull)
            change = jnp.dot(
                zmat[...], jnp.concatenate([high, low, high], axis=0), preferred_element_type=F32
            )
            v[:, lanes] = v[:, lanes] + change
            f[:, lanes] = fp[:, lanes] + DT * change
            if advance:
                p[:, lanes] = tp[:, lanes] - (DT * ratio[0:1, lanes]) * change[0:RIM, :]

    def cross_copy(turn, b, t):
        return pltpu.make_async_remote_copy(
            src_ref=xs.at[turn, b * SUBS + t],
            dst_ref=xr.at[turn, (GROUPS - 2 - b) * SUBS + s],
            send_sem=xs_sem.at[turn],
            recv_sem=xr_sem.at[turn],
            device_id=(lax.rem(g + 1 + b, GROUPS), t),
            device_id_type=MESH,
        )

    def side_copy(turn, side):
        return pltpu.make_async_remote_copy(
            src_ref=ns.at[turn, side],
            dst_ref=nr.at[turn, 1 - side],
            send_sem=ns_sem.at[turn, side],
            recv_sem=nr_sem.at[turn, 1 - side],
            device_id=(g, down if side else up),
            device_id_type=MESH,
        )

    blank = jnp.zeros((LANES - 2 * RIM, LANES), F32)

    def send(turn):
        for block in range((GROUPS - 1) * SUBS * SLOT // LANES):
            lanes = pl.ds((2 + block) * LANES, LANES)
            tile = jnp.concatenate([f[0:RIM, lanes], fp[0:RIM, lanes], blank], axis=0)
            per = LANES // SLOT
            xs[turn, block * per : (block + 1) * per, :, :] = tile.T.reshape(per, SLOT, LANES)
        for side in range(2):
            lanes = pl.ds(side * LANES, LANES)
            ns[turn, side, 0:RIM, :] = f[0:RIM, lanes]
            ns[turn, side, RIM:, :] = fp[0:RIM, lanes]

        def go(k, carry):
            t = lax.rem(s + k, SUBS)
            for b in range(GROUPS - 1):
                cross_copy(turn, b, t).start()
            return carry

        lax.fori_loop(0, SUBS, go, 0)
        for side in range(2):
            side_copy(turn, side).start()

    def receive(turn):
        for side in range(2):
            side_copy(turn, 1 - side).wait_recv()
            lanes = pl.ds(side * LANES, LANES)
            p[:, lanes] = nr[turn, side, 0:RIM, :]
            tp[:, lanes] = nr[turn, side, RIM:, :]
        pltpu.make_async_copy(xr.at[turn], xr.at[turn], xr_sem.at[turn]).wait()
        for block in range((GROUPS - 1) * SUBS * SLOT // LANES):
            lanes = pl.ds((2 + block) * LANES, LANES)
            per = LANES // SLOT
            tile = xr[turn, block * per : (block + 1) * per, :, :].reshape(LANES, LANES).T
            p[:, lanes] = tile[0:RIM, :]
            tp[:, lanes] = tile[RIM : 2 * RIM, :]

    local()
    pl.semaphore_wait(barrier, (GROUPS - 1) * SUBS + 2)

    def pair(turn, carry):
        @pl.when(turn > 0)
        def _():
            local()

        send(turn)
        receive(turn)
        ratio[...] = p[FN : FN + 1, :] * jac_ref[...].reshape(1, elements)
        rim(True)
        local()
        rim(False)
        return carry

    lax.fori_loop(0, ROUNDS - 1, pair, 0)
    send(ROUNDS - 1)
    local()
    receive(ROUNDS - 1)
    rim(False)

    for source, target in ((f, od_ref), (v, ov_ref)):
        for c in range(3):
            target[c, 0:FN, :] = source[16 * c : 16 * c + FN, :]
            target[c, FN:NODES, :] = source[RIM + REST * c : RIM + REST * (c + 1), :]
    for turn in range(ROUNDS):
        pltpu.make_async_copy(xs.at[turn], xs.at[turn], xs_sem.at[turn]).wait()
        for side in range(2):
            side_copy(turn, side).wait_send()


def shards(*args):
    elements = args[0].shape[2]
    consts = tuple(jnp.asarray(t) for t in tables())
    shape = jax.ShapeDtypeStruct(args[0].shape, F32)
    slots = (GROUPS - 1) * SUBS
    vmem = pl.BlockSpec(memory_space=pltpu.VMEM)
    return pl.pallas_call(
        kernel,
        out_shape=(shape, shape),
        in_specs=[vmem] * (len(args) + len(consts)),
        out_specs=(vmem, vmem),
        scratch_shapes=[
            pltpu.VMEM((ROWS, elements), F32),
            pltpu.VMEM((ROWS, elements), F32),
            pltpu.VMEM((ROWS, elements), F32),
            pltpu.VMEM((RIM, elements), F32),
            pltpu.VMEM((RIM, elements), F32),
            pltpu.VMEM((PIECES * ROWS + 3 * RIM, 3 * ROWS), BF16),
            pltpu.VMEM((ROWS, 9 * RIM), BF16),
            pltpu.VMEM((ROWS, 3 * RIM), BF16),
            pltpu.VMEM((PIECES, elements), F32),
            pltpu.VMEM((1, elements), F32),
            pltpu.VMEM((3, 5, elements), F32),
            pltpu.VMEM((3, 2, elements), jnp.int32),
            pltpu.VMEM((5, elements), F32),
            pltpu.VMEM((ROUNDS, slots, SLOT, LANES), F32),
            pltpu.VMEM((ROUNDS, slots, SLOT, LANES), F32),
            pltpu.VMEM((ROUNDS, 2, 2 * RIM, LANES), F32),
            pltpu.VMEM((ROUNDS, 2, 2 * RIM, LANES), F32),
            pltpu.SemaphoreType.DMA((ROUNDS,)),
            pltpu.SemaphoreType.DMA((ROUNDS,)),
            pltpu.SemaphoreType.DMA((ROUNDS, 2)),
            pltpu.SemaphoreType.DMA((ROUNDS, 2)),
        ],
        compiler_params=pltpu.CompilerParams(collective_id=0, has_side_effects=True),
    )(*args, *consts)


def solution(mesh):
    lanes = P(None, ("group", "sub"))
    state = P(None, None, ("group", "sub"))
    flat = P(("group", "sub"))
    return jax.shard_map(
        shards,
        mesh=mesh,
        in_specs=(state, state, lanes, flat, P(), P(), P(), lanes, lanes, lanes, lanes, flat, lanes),
        out_specs=(state, state),
        check_vma=False,
    )
```

```python
import functools

import jax
import jax.numpy as jnp
import numpy as np
from jax import lax
from jax.experimental import pallas as pl
from jax.experimental.pallas import tpu as pltpu
from jax.sharding import PartitionSpec as P

MESH = pl.DeviceIdType.MESH
HIGHEST = lax.Precision.HIGHEST
F32 = jnp.float32
BF16 = jnp.bfloat16

DT = 0.25
NODES = 35
FN = 15
LANES = 128
ROWS = 112
RIM = 48
REST = NODES - FN
PIECES = 6
GROUPS = 4
SUBS = 32
SLOT = 8
ROUNDS = 3


def row_of(c, n):
    return 16 * c + n if n < FN else RIM + REST * c + n - FN


def tables():
    points = [(a, b, c, 4 - a - b - c) for a in range(5) for b in range(5 - a) for c in range(5 - a - b)]
    faces = [[i for i, p in enumerate(points) if p[k] == 0] for k in range(4)]
    spread = np.zeros((ROWS, NODES), np.float32)
    perm = np.zeros((3 * NODES, ROWS), np.float32)
    select = np.zeros((4 * RIM, ROWS), np.float32)
    place = np.zeros((FN, 4 * RIM), np.float32)
    comp = np.full((ROWS,), -1, np.int64)
    for c in range(3):
        for n in range(NODES):
            spread[row_of(c, n), n] = 1.0
            perm[c * NODES + n, row_of(c, n)] = 1.0
            comp[row_of(c, n)] = c
        for k in range(4):
            for i, n in enumerate(faces[k]):
                select[k * RIM + 16 * c + i, row_of(c, n)] = 1.0
                place[i, k * RIM + 16 * c + i] = 1.0
    same = ((comp[:, None] == comp[None, :]) & (comp[:, None] >= 0)).astype(np.float32)
    block = np.arange(4 * RIM) // 16
    same_face = (block[:, None] == block[None, :]).astype(np.float32)
    return spread, perm, select, place, same, same_face


def dot(a, b, dims=((1,), (0,))):
    return lax.dot_general(a, b, (dims, ((), ())), precision=HIGHEST, preferred_element_type=F32)


def halves(x):
    high = x.astype(BF16)
    return high, (x - high.astype(F32)).astype(BF16)


def traction(j, u, rigid, soft):
    jn = u[0] * j[0] + u[1] * j[1] + u[2] * j[2]
    size = j[0] * j[0] + j[1] * j[1] + j[2] * j[2] + jn * jn
    e = soft * jnp.exp(size * -0.125)
    a = rigid + e
    b = e * jn
    return [a * j[c] + b * u[c] for c in range(3)]


def kernel(
    d_ref, v_ref, w_ref, jac_ref, s_ref, fm_ref, mi_ref, ll_ref, lg_ref, nl_ref, ng_ref, cl_ref, cg_ref,
    spread_ref, perm_ref, select_ref, place_ref, same_ref, face_ref,
    od_ref, ov_ref,
    f, v, fp, p, tp, amat, smat, lmat, zmat, fh, tr, th, wj, ratio, lc, li, zc,
    xs, xr, ns, nr, xs_sem, xr_sem, ns_sem, nr_sem,
):
    g = lax.axis_index("group")
    s = lax.axis_index("sub")
    elements = f.shape[1]
    up = lax.rem(s + 1, SUBS)
    down = lax.rem(s + SUBS - 1, SUBS)
    barrier = pltpu.get_barrier_semaphore()

    def greet(t, carry):
        for b in range(GROUPS - 1):
            pl.semaphore_signal(
                barrier, inc=1, device_id=(lax.rem(g + 1 + b, GROUPS), t), device_id_type=MESH
            )
        return carry

    lax.fori_loop(0, SUBS, greet, 0)
    for t in (up, down):
        pl.semaphore_signal(barrier, inc=1, device_id=(g, t), device_id_type=MESH)

    jac = jac_ref[...].reshape(1, elements)
    inv = 1.0 / jac
    wj[...] = w_ref[...] * (inv * -DT)
    for q in range(3):
        part = pl.ds(q * elements, elements)
        state = ll_ref[1:2, part]
        scale = lg_ref[3:4, part] * (inv * DT)
        lc[q, 0:3, :] = lg_ref[0:3, part]
        lc[q, 3:4, :] = jnp.where(state == 0, scale, 0.0)
        lc[q, 4:5, :] = jnp.where(state == 1, 0.5 * scale, 0.0)
        partner = ll_ref[0:1, part]
        li[q, 0:1, :] = lax.rem(partner, LANES)
        li[q, 1:2, :] = lax.div(partner, LANES)
    cross = elements - 2 * LANES
    spots = (
        (0, LANES, ng_ref[0:4, :], nl_ref[0:1, :]),
        (LANES, LANES, ng_ref[4:8, :], nl_ref[1:2, :]),
        (2 * LANES, cross, cg_ref[...], cl_ref[...].reshape(1, cross)),
    )
    for at, size, geometry, state in spots:
        lanes = pl.ds(at, size)
        scale = geometry[3:4, :] * (inv[:, at : at + size] * DT)
        zc[0:3, lanes] = geometry[0:3, :]
        zc[3:4, lanes] = jnp.where(state == 0, scale, 0.0)
        zc[4:5, lanes] = jnp.where(state == 1, 0.5 * scale, 0.0)

    for source, target in ((d_ref, f), (v_ref, v)):
        for c in range(3):
            target[16 * c : 16 * c + FN, :] = source[c, 0:FN, :]
            target[16 * c + FN : 16 * c + FN + 1, :] = jnp.zeros((1, elements), F32)
            target[RIM + REST * c : RIM + REST * (c + 1), :] = source[c, FN:NODES, :]
        target[RIM + 3 * REST :, :] = jnp.zeros((ROWS - RIM - 3 * REST, elements), F32)
    f[FN : FN + 1, :] = inv

    spread = spread_ref[...]
    mass = dot(dot(spread, mi_ref[...]), spread, ((1,), (1,))) * same_ref[...]
    place = place_ref[...]
    face = dot(dot(place, fm_ref[...], ((0,), (0,))), place) * face_ref[...]
    lift = dot(mass, dot(select_ref[...], face, ((0,), (0,))))
    high, low = halves(lift)
    zmat[:, 0:RIM] = high[:, 0:RIM]
    zmat[:, RIM : 2 * RIM] = high[:, 0:RIM]
    zmat[:, 2 * RIM : 3 * RIM] = low[:, 0:RIM]
    lmat[:, 0 : 3 * RIM] = high[:, RIM:]
    lmat[:, 3 * RIM : 6 * RIM] = high[:, RIM:]
    lmat[:, 6 * RIM : 9 * RIM] = low[:, RIM:]
    turned = dot(perm_ref[...], s_ref[...], ((0,), (0,)))
    for m in range(PIECES):
        piece = turned[:, m * 3 * NODES : (m + 1) * 3 * NODES]
        high, low = halves(dot(mass, dot(piece, piece, ((1,), (1,)))))
        rows = slice(m * ROWS, (m + 1) * ROWS)
        amat[rows, 0:ROWS] = high
        amat[rows, ROWS : 2 * ROWS] = high
        amat[rows, 2 * ROWS : 3 * ROWS] = low
    chosen = select_ref[RIM:, :].astype(BF16)
    smat[:, 0:ROWS] = chosen
    smat[:, ROWS : 2 * ROWS] = chosen

    def local(width=2 * LANES):
        for at in range(0, elements, width):
            lanes = pl.ds(at, width)
            high, low = halves(f[:, lanes])
            fh[0:ROWS, lanes] = high
            fh[ROWS : 2 * ROWS, lanes] = low
            fh[2 * ROWS :, lanes] = high
            tr[:, lanes] = jnp.dot(smat[...], fh[0 : 2 * ROWS, lanes], preferred_element_type=F32)
        for at in range(0, elements, width):
            lanes = pl.ds(at, width)
            product = jnp.dot(amat[...], fh[:, lanes], preferred_element_type=F32)
            change = wj[0:1, lanes] * product[0:ROWS, :]
            for m in range(1, PIECES):
                change = change + wj[m : m + 1, lanes] * product[m * ROWS : (m + 1) * ROWS, :]
            v[:, lanes] = v[:, lanes] + change
            for block in range(at, at + width, LANES):
                pull(block)
        for at in range(0, elements, width):
            lanes = pl.ds(at, width)
            speed = v[:, lanes] + jnp.dot(lmat[...], th[:, lanes], preferred_element_type=F32)
            v[:, lanes] = speed
            fp[:, lanes] = f[:, lanes] + DT * speed

    def pull(block):
        here = pl.ds(block, LANES)
        for q in range(3):
            index = jnp.broadcast_to(li[q, 0:1, here], (16, LANES))
            origin = jnp.broadcast_to(li[q, 1:2, here], (16, LANES))
            jump = []
            for c in range(3):
                found = [
                    jnp.take_along_axis(
                        tr[r * RIM + 16 * c : r * RIM + 16 * (c + 1), here], index, axis=1, mode="promise_in_bounds"
                    )
                    for r in range(3)
                ]
                paired = jnp.where(origin == 0, found[0], jnp.where(origin == 1, found[1], found[2]))
                jump.append(paired - tr[q * RIM + 16 * c : q * RIM + 16 * (c + 1), here])
            parts = traction(
                jump, [lc[q, c : c + 1, here] for c in range(3)], lc[q, 3:4, here], lc[q, 4:5, here]
            )
            for c in range(3):
                high, low = halves(parts[c])
                at = q * RIM + 16 * c
                th[at : at + 16, here] = high
                th[3 * RIM + at : 3 * RIM + at + 16, here] = low
                th[6 * RIM + at : 6 * RIM + at + 16, here] = high

    def rim(advance, width=2 * LANES):
        for at in range(0, elements, width):
            lanes = pl.ds(at, width)
            jump = p[:, lanes] - f[0:RIM, lanes]
            pull = jnp.concatenate(
                traction(
                    [jump[16 * c : 16 * (c + 1), :] for c in range(3)],
                    [zc[c : c + 1, lanes] for c in range(3)],
                    zc[3:4, lanes],
                    zc[4:5, lanes],
                ),
                axis=0,
            )
            high, low = halves(pull)
            change = jnp.dot(
                zmat[...], jnp.concatenate([high, low, high], axis=0), preferred_element_type=F32
            )
            v[:, lanes] = v[:, lanes] + change
            f[:, lanes] = fp[:, lanes] + DT * change
            if advance:
                p[:, lanes] = tp[:, lanes] - (DT * ratio[0:1, lanes]) * change[0:RIM, :]

    def cross_copy(turn, b, t):
        return pltpu.make_async_remote_copy(
            src_ref=xs.at[turn, b * SUBS + t],
            dst_ref=xr.at[turn, (GROUPS - 2 - b) * SUBS + s],
            send_sem=xs_sem.at[turn],
            recv_sem=xr_sem.at[turn],
            device_id=(lax.rem(g + 1 + b, GROUPS), t),
            device_id_type=MESH,
        )

    def side_copy(turn, side):
        return pltpu.make_async_remote_copy(
            src_ref=ns.at[turn, side],
            dst_ref=nr.at[turn, 1 - side],
            send_sem=ns_sem.at[turn, side],
            recv_sem=nr_sem.at[turn, 1 - side],
            device_id=(g, down if side else up),
            device_id_type=MESH,
        )

    blank = jnp.zeros((LANES - 2 * RIM, LANES), F32)

    def send(turn):
        for block in range((GROUPS - 1) * SUBS * SLOT // LANES):
            lanes = pl.ds((2 + block) * LANES, LANES)
            tile = jnp.concatenate([f[0:RIM, lanes], fp[0:RIM, lanes], blank], axis=0)
            per = LANES // SLOT
            xs[turn, block * per : (block + 1) * per, :, :] = tile.T.reshape(per, SLOT, LANES)
        for side in range(2):
            lanes = pl.ds(side * LANES, LANES)
            ns[turn, side, 0:RIM, :] = f[0:RIM, lanes]
            ns[turn, side, RIM:, :] = fp[0:RIM, lanes]

        def go(k, carry):
            t = lax.rem(s + k, SUBS)
            for b in range(GROUPS - 1):
                cross_copy(turn, b, t).start()
            return carry

        lax.fori_loop(0, SUBS, go, 0)
        for side in range(2):
            side_copy(turn, side).start()

    def receive(turn):
        for side in range(2):
            side_copy(turn, 1 - side).wait_recv()
            lanes = pl.ds(side * LANES, LANES)
            p[:, lanes] = nr[turn, side, 0:RIM, :]
            tp[:, lanes] = nr[turn, side, RIM:, :]
        pltpu.make_async_copy(xr.at[turn], xr.at[turn], xr_sem.at[turn]).wait()
        for block in range((GROUPS - 1) * SUBS * SLOT // LANES):
            lanes = pl.ds((2 + block) * LANES, LANES)
            per = LANES // SLOT
            tile = xr[turn, block * per : (block + 1) * per, :, :].reshape(LANES, LANES).T
            p[:, lanes] = tile[0:RIM, :]
            tp[:, lanes] = tile[RIM : 2 * RIM, :]

    local()
    pl.semaphore_wait(barrier, (GROUPS - 1) * SUBS + 2)

    def pair(turn, carry):
        @pl.when(turn > 0)
        def _():
            local()

        send(turn)
        receive(turn)
        ratio[...] = p[FN : FN + 1, :] * jac_ref[...].reshape(1, elements)
        rim(True)
        local()
        rim(False)
        return carry

    lax.fori_loop(0, ROUNDS - 1, pair, 0)
    send(ROUNDS - 1)
    local()
    receive(ROUNDS - 1)
    rim(False)

    for source, target in ((f, od_ref), (v, ov_ref)):
        for c in range(3):
            target[c, 0:FN, :] = source[16 * c : 16 * c + FN, :]
            target[c, FN:NODES, :] = source[RIM + REST * c : RIM + REST * (c + 1), :]
    for turn in range(ROUNDS):
        pltpu.make_async_copy(xs.at[turn], xs.at[turn], xs_sem.at[turn]).wait()
        for side in range(2):
            side_copy(turn, side).wait_send()


def shards(*args):
    elements = args[0].shape[2]
    args = args[:4] + (args[4].T,) + args[5:]
    consts = tuple(jnp.asarray(t) for t in tables())
    shape = jax.ShapeDtypeStruct(args[0].shape, F32)
    slots = (GROUPS - 1) * SUBS
    vmem = pl.BlockSpec(memory_space=pltpu.VMEM)
    return pl.pallas_call(
        kernel,
        out_shape=(shape, shape),
        in_specs=[vmem] * (len(args) + len(consts)),
        out_specs=(vmem, vmem),
        scratch_shapes=[
            pltpu.VMEM((ROWS, elements), F32),
            pltpu.VMEM((ROWS, elements), F32),
            pltpu.VMEM((ROWS, elements), F32),
            pltpu.VMEM((RIM, elements), F32),
            pltpu.VMEM((RIM, elements), F32),
            pltpu.VMEM((PIECES * ROWS, 3 * ROWS), BF16),
            pltpu.VMEM((3 * RIM, 2 * ROWS), BF16),
            pltpu.VMEM((ROWS, 9 * RIM), BF16),
            pltpu.VMEM((ROWS, 3 * RIM), BF16),
            pltpu.VMEM((3 * ROWS, elements), BF16),
            pltpu.VMEM((3 * RIM, elements), F32),
            pltpu.VMEM((9 * RIM, elements), BF16),
            pltpu.VMEM((PIECES, elements), F32),
            pltpu.VMEM((1, elements), F32),
            pltpu.VMEM((3, 5, elements), F32),
            pltpu.VMEM((3, 2, elements), jnp.int32),
            pltpu.VMEM((5, elements), F32),
            pltpu.VMEM((ROUNDS, slots, SLOT, LANES), F32),
            pltpu.VMEM((ROUNDS, slots, SLOT, LANES), F32),
            pltpu.VMEM((ROUNDS, 2, 2 * RIM, LANES), F32),
            pltpu.VMEM((ROUNDS, 2, 2 * RIM, LANES), F32),
            pltpu.SemaphoreType.DMA((ROUNDS,)),
            pltpu.SemaphoreType.DMA((ROUNDS,)),
            pltpu.SemaphoreType.DMA((ROUNDS, 2)),
            pltpu.SemaphoreType.DMA((ROUNDS, 2)),
        ],
        compiler_params=pltpu.CompilerParams(collective_id=0, has_side_effects=True),
    )(*args, *consts)


def solution(mesh):
    lanes = P(None, ("group", "sub"))
    state = P(None, None, ("group", "sub"))
    flat = P(("group", "sub"))
    return jax.shard_map(
        shards,
        mesh=mesh,
        in_specs=(state, state, lanes, flat, P(), P(), P(), lanes, lanes, lanes, lanes, flat, lanes),
        out_specs=(state, state),
        check_vma=False,
    )
```

```python
import functools

import jax
import jax.numpy as jnp
import numpy as np
from jax import lax
from jax.experimental import pallas as pl
from jax.experimental.pallas import tpu as pltpu
from jax.sharding import PartitionSpec as P

MESH = pl.DeviceIdType.MESH
HIGHEST = lax.Precision.HIGHEST
F32 = jnp.float32
BF16 = jnp.bfloat16

DT = 0.25
NODES = 35
FN = 15
LANES = 128
ROWS = 112
RIM = 48
REST = NODES - FN
PIECES = 6
GROUPS = 4
SUBS = 32
SLOT = 8
ROUNDS = 3
MESSAGES = 2 * ROUNDS - 1
LINES = 3
NAMES = (
    "displacement", "velocity", "weights", "jacobian", "strain", "face_mass", "mass", "local_links", "local_geometry",
    "side_links", "side_geometry", "cross_links", "cross_geometry",
    "spread", "perm", "select", "place", "same", "face",
)


def row_of(c, n):
    return 16 * c + n if n < FN else RIM + REST * c + n - FN


def tables():
    points = [(a, b, c, 4 - a - b - c) for a in range(5) for b in range(5 - a) for c in range(5 - a - b)]
    faces = [[i for i, p in enumerate(points) if p[k] == 0] for k in range(4)]
    spread = np.zeros((ROWS, NODES), np.float32)
    perm = np.zeros((3 * NODES, ROWS), np.float32)
    select = np.zeros((4 * RIM, ROWS), np.float32)
    place = np.zeros((FN, 4 * RIM), np.float32)
    comp = np.full((ROWS,), -1, np.int64)
    for c in range(3):
        for n in range(NODES):
            spread[row_of(c, n), n] = 1.0
            perm[c * NODES + n, row_of(c, n)] = 1.0
            comp[row_of(c, n)] = c
        for k in range(4):
            for i, n in enumerate(faces[k]):
                select[k * RIM + 16 * c + i, row_of(c, n)] = 1.0
                place[i, k * RIM + 16 * c + i] = 1.0
    same = ((comp[:, None] == comp[None, :]) & (comp[:, None] >= 0)).astype(np.float32)
    block = np.arange(4 * RIM) // 16
    same_face = (block[:, None] == block[None, :]).astype(np.float32)
    return spread, perm, select, place, same, same_face


def dot(a, b, dims=((1,), (0,))):
    return lax.dot_general(a, b, (dims, ((), ())), precision=HIGHEST, preferred_element_type=F32)


def halves(x):
    high = x.astype(BF16)
    return high, (x - high.astype(F32)).astype(BF16)


def traction(j, u, rigid, soft):
    jn = u[0] * j[0] + u[1] * j[1] + u[2] * j[2]
    size = j[0] * j[0] + j[1] * j[1] + j[2] * j[2] + jn * jn
    e = soft * jnp.exp(size * -0.125)
    a = rigid + e
    b = e * jn
    return [a * j[c] + b * u[c] for c in range(3)]


def kernel(*refs):
    count = len(NAMES)
    hbm = refs[:count]
    ovp, ofp, oc = refs[count : count + 3]
    buffers = refs[count + 3 : 2 * count + 3]
    (
        f, v, fp, p, ch, amat, smat, lmat, zmat, fh, tr, th, wj, ratio, lc, li, zc,
        xs, xr, ns, nr, in_sem, xs_sem, xr_sem, ns_sem, nr_sem,
    ) = refs[2 * count + 3 :]
    (
        d_ref, v_ref, w_ref, jac_ref, s_ref, fm_ref, mi_ref, ll_ref, lg_ref, nl_ref, ng_ref, cl_ref, cg_ref,
        spread_ref, perm_ref, select_ref, place_ref, same_ref, face_ref,
    ) = buffers
    loads = [pltpu.make_async_copy(hbm[k], buffers[k], in_sem.at[k]) for k in range(count)]
    g = lax.axis_index("group")
    s = lax.axis_index("sub")
    elements = f.shape[1]
    up = lax.rem(s + 1, SUBS)
    down = lax.rem(s + SUBS - 1, SUBS)
    barrier = pltpu.get_barrier_semaphore()

    def greet(t, carry):
        for b in range(GROUPS - 1):
            pl.semaphore_signal(
                barrier, inc=1, device_id=(lax.rem(g + 1 + b, GROUPS), t), device_id_type=MESH
            )
        return carry

    lax.fori_loop(0, SUBS, greet, 0)
    for t in (up, down):
        pl.semaphore_signal(barrier, inc=1, device_id=(g, t), device_id_type=MESH)
    first = (NAMES.index("displacement"), NAMES.index("jacobian"))
    for k in first:
        loads[k].start()
    for k in range(count):
        if k not in first:
            loads[k].start()

    def fill(source, target):
        for c in range(3):
            target[16 * c : 16 * c + FN, :] = source[c, 0:FN, :]
            target[16 * c + FN : 16 * c + FN + 1, :] = jnp.zeros((1, elements), F32)
            target[RIM + REST * c : RIM + REST * (c + 1), :] = source[c, FN:NODES, :]
        target[RIM + 3 * REST :, :] = jnp.zeros((ROWS - RIM - 3 * REST, elements), F32)

    for k in first:
        loads[k].wait()
    jac = jac_ref[...].reshape(1, elements)
    inv = 1.0 / jac
    fill(d_ref, f)
    f[FN : FN + 1, :] = inv

    def cross_copy(turn, b, t):
        return pltpu.make_async_remote_copy(
            src_ref=xs.at[turn, b * SUBS + t],
            dst_ref=xr.at[turn, (GROUPS - 2 - b) * SUBS + s],
            send_sem=xs_sem.at[turn],
            recv_sem=xr_sem.at[turn],
            device_id=(lax.rem(g + 1 + b, GROUPS), t),
            device_id_type=MESH,
        )

    def side_copy(turn, side):
        return pltpu.make_async_remote_copy(
            src_ref=ns.at[turn, side],
            dst_ref=nr.at[turn, 1 - side],
            send_sem=ns_sem.at[turn, side],
            recv_sem=nr_sem.at[turn, 1 - side],
            device_id=(g, down if side else up),
            device_id_type=MESH,
        )

    per = LANES // SLOT
    slot = lax.rem(lax.broadcasted_iota(jnp.int32, (8, LANES), 1), SLOT)

    def shift(x, by):
        return pltpu.roll(x, by % LANES, 1) if by % LANES else x

    def pack(turn, source):
        for block in range((GROUPS - 1) * SUBS // per):
            lanes = pl.ds((2 + block) * LANES, LANES)
            x = [source[8 * k : 8 * k + 8, lanes] for k in range(6)]
            tile = x + [shift(x[k], -3) for k in range(6)]
            for k in range(4):
                parts = []
                for r in range(3):
                    i = 4 * r + k
                    parts.append(shift(x[i % 6], r - (6 + i // 6)))
                tile.append(jnp.where(slot == 0, parts[0], jnp.where(slot == 1, parts[1], parts[2])))
            turned = jnp.concatenate(tile, axis=0).T.reshape(per, SLOT, LANES)
            xs[turn, block * per : (block + 1) * per, :, :] = turned[:, 0:LINES, :]
        for side in range(2):
            ns[turn, side, :, :] = source[0:RIM, pl.ds(side * LANES, LANES)]

    def send(turn):
        def go(k, carry):
            t = lax.rem(s + k, SUBS)
            for b in range(GROUPS - 1):
                cross_copy(turn, b, t).start()
            return carry

        lax.fori_loop(0, SUBS, go, 0)
        for side in range(2):
            side_copy(turn, side).start()

    def receive(turn, target):
        for side in range(2):
            side_copy(turn, 1 - side).wait_recv()
            target[:, pl.ds(side * LANES, LANES)] = nr[turn, side, :, :]
        pltpu.make_async_copy(xr.at[turn], xr.at[turn], xr_sem.at[turn]).wait()
        for block in range((GROUPS - 1) * SUBS // per):
            lanes = pl.ds((2 + block) * LANES, LANES)
            rows = xr[turn, block * per : (block + 1) * per, :, :]
            rows = jnp.concatenate([rows, jnp.zeros((per, SLOT - LINES, LANES), F32)], axis=1)
            tile = rows.reshape(LANES, LANES).T
            for k in range(6):
                x = tile[8 * k : 8 * k + 8, :]
                y = shift(tile[RIM + 8 * k : RIM + 8 * k + 8, :], 3)
                late = []
                for q in range(2):
                    i = 6 * q + k
                    at = 2 * RIM + 8 * (i % 4)
                    late.append(shift(tile[at : at + 8, :], 6 + q - i // 4))
                y = jnp.where(slot < 6, y, jnp.where(slot == 6, late[0], late[1]))
                target[8 * k : 8 * k + 8, lanes] = jnp.where(slot < 3, x, y)

    def empty(source, target):
        for c in range(3):
            target[c, 0:FN, :] = source[16 * c : 16 * c + FN, :]
            target[c, FN:NODES, :] = source[RIM + REST * c : RIM + REST * (c + 1), :]

    pack(0, f)
    pl.semaphore_wait(barrier, (GROUPS - 1) * SUBS + 2)
    send(0)

    for k in range(count):
        if k not in first:
            loads[k].wait()
    fill(v_ref, v)

    wj[...] = w_ref[...] * (inv * -DT)
    for q in range(3):
        part = pl.ds(q * elements, elements)
        state = ll_ref[1:2, part]
        scale = lg_ref[3:4, part] * (inv * DT)
        lc[q, 0:3, :] = lg_ref[0:3, part]
        lc[q, 3:4, :] = jnp.where(state == 0, scale, 0.0)
        lc[q, 4:5, :] = jnp.where(state == 1, 0.5 * scale, 0.0)
        partner = ll_ref[0:1, part]
        li[q, 0:1, :] = lax.rem(partner, LANES)
        li[q, 1:2, :] = lax.div(partner, LANES)
    cross = elements - 2 * LANES
    spots = (
        (0, LANES, ng_ref[0:4, :], nl_ref[0:1, :]),
        (LANES, LANES, ng_ref[4:8, :], nl_ref[1:2, :]),
        (2 * LANES, cross, cg_ref[...], cl_ref[...].reshape(1, cross)),
    )
    for at, size, geometry, state in spots:
        lanes = pl.ds(at, size)
        scale = geometry[3:4, :] * (inv[:, at : at + size] * DT)
        zc[0:3, lanes] = geometry[0:3, :]
        zc[3:4, lanes] = jnp.where(state == 0, scale, 0.0)
        zc[4:5, lanes] = jnp.where(state == 1, 0.5 * scale, 0.0)

    spread = spread_ref[...]
    mass = dot(dot(spread, mi_ref[...]), spread, ((1,), (1,))) * same_ref[...]
    place = place_ref[...]
    face = dot(dot(place, fm_ref[...], ((0,), (0,))), place) * face_ref[...]
    lift = dot(mass, dot(select_ref[...], face, ((0,), (0,))))
    high, low = halves(lift)
    zmat[:, 0:RIM] = high[:, 0:RIM]
    zmat[:, RIM : 2 * RIM] = high[:, 0:RIM]
    zmat[:, 2 * RIM : 3 * RIM] = low[:, 0:RIM]
    lmat[:, 0 : 3 * RIM] = high[:, RIM:]
    lmat[:, 3 * RIM : 6 * RIM] = high[:, RIM:]
    lmat[:, 6 * RIM : 9 * RIM] = low[:, RIM:]
    turned = dot(perm_ref[...], s_ref[...], ((0,), (0,)))
    for m in range(PIECES):
        piece = turned[:, m * 3 * NODES : (m + 1) * 3 * NODES]
        high, low = halves(dot(mass, dot(piece, piece, ((1,), (1,)))))
        rows = slice(m * ROWS, (m + 1) * ROWS)
        amat[rows, 0:ROWS] = high
        amat[rows, ROWS : 2 * ROWS] = high
        amat[rows, 2 * ROWS : 3 * ROWS] = low
    chosen = select_ref[RIM:, :].astype(BF16)
    smat[:, 0:ROWS] = chosen
    smat[:, ROWS : 2 * ROWS] = chosen

    def local(width=2 * LANES):
        for at in range(0, elements, width):
            lanes = pl.ds(at, width)
            high, low = halves(f[:, lanes])
            fh[0:ROWS, lanes] = high
            fh[ROWS : 2 * ROWS, lanes] = low
            fh[2 * ROWS :, lanes] = high
            tr[:, lanes] = jnp.dot(smat[...], fh[0 : 2 * ROWS, lanes], preferred_element_type=F32)
        for at in range(0, elements, width):
            lanes = pl.ds(at, width)
            product = jnp.dot(amat[...], fh[:, lanes], preferred_element_type=F32)
            change = wj[0:1, lanes] * product[0:ROWS, :]
            for m in range(1, PIECES):
                change = change + wj[m : m + 1, lanes] * product[m * ROWS : (m + 1) * ROWS, :]
            v[:, lanes] = v[:, lanes] + change
            for block in range(at, at + width, LANES):
                pull(block)
        for at in range(0, elements, width):
            lanes = pl.ds(at, width)
            speed = v[:, lanes] + jnp.dot(lmat[...], th[:, lanes], preferred_element_type=F32)
            v[:, lanes] = speed
            fp[:, lanes] = f[:, lanes] + DT * speed

    def pull(block):
        here = pl.ds(block, LANES)
        for q in range(3):
            index = jnp.broadcast_to(li[q, 0:1, here], (16, LANES))
            origin = jnp.broadcast_to(li[q, 1:2, here], (16, LANES))
            jump = []
            for c in range(3):
                found = [
                    jnp.take_along_axis(
                        tr[r * RIM + 16 * c : r * RIM + 16 * (c + 1), here], index, axis=1, mode="promise_in_bounds"
                    )
                    for r in range(3)
                ]
                paired = jnp.where(origin == 0, found[0], jnp.where(origin == 1, found[1], found[2]))
                jump.append(paired - tr[q * RIM + 16 * c : q * RIM + 16 * (c + 1), here])
            parts = traction(
                jump, [lc[q, c : c + 1, here] for c in range(3)], lc[q, 3:4, here], lc[q, 4:5, here]
            )
            for c in range(3):
                high, low = halves(parts[c])
                at = q * RIM + 16 * c
                th[at : at + 16, here] = high
                th[3 * RIM + at : 3 * RIM + at + 16, here] = low
                th[6 * RIM + at : 6 * RIM + at + 16, here] = high

    def rim(keep, last=False, width=2 * LANES):
        for at in range(0, elements, width):
            lanes = pl.ds(at, width)
            jump = p[:, lanes] - f[0:RIM, lanes]
            pulled = jnp.concatenate(
                traction(
                    [jump[16 * c : 16 * (c + 1), :] for c in range(3)],
                    [zc[c : c + 1, lanes] for c in range(3)],
                    zc[3:4, lanes],
                    zc[4:5, lanes],
                ),
                axis=0,
            )
            high, low = halves(pulled)
            change = jnp.dot(
                zmat[...], jnp.concatenate([high, low, high], axis=0), preferred_element_type=F32
            )
            if last:
                f[:, lanes] = change
                continue
            v[:, lanes] = v[:, lanes] + change
            f[:, lanes] = fp[:, lanes] + DT * change
            if keep:
                ch[:, lanes] = change[0:RIM, :]

    def pair(turn, carry):
        local()
        pack(2 * turn + 1, fp)
        send(2 * turn + 1)
        receive(2 * turn, p)
        ratio[...] = p[FN : FN + 1, :] * (jac_ref[...].reshape(1, elements) * -DT)
        rim(True)
        local()
        receive(2 * turn + 1, p)
        for at in range(0, elements, 2 * LANES):
            lanes = pl.ds(at, 2 * LANES)
            p[:, lanes] = p[:, lanes] + ratio[0:1, lanes] * ch[:, lanes]
        rim(False)
        pack(2 * turn + 2, f)
        send(2 * turn + 2)
        return carry

    lax.fori_loop(0, ROUNDS - 1, pair, 0)
    local()
    empty(v, ovp)
    empty(fp, ofp)
    receive(2 * ROUNDS - 2, p)
    rim(False, True)
    empty(f, oc)
    for turn in range(MESSAGES):
        pltpu.make_async_copy(xs.at[turn], xs.at[turn], xs_sem.at[turn]).wait()
        for side in range(2):
            side_copy(turn, side).wait_send()


def shards(*args):
    elements = args[0].shape[2]
    shape = jax.ShapeDtypeStruct(args[0].shape, F32)
    args = args[:4] + (args[4].T,) + args[5:] + tuple(jnp.asarray(t) for t in tables())
    slots = (GROUPS - 1) * SUBS
    vmem = pl.BlockSpec(memory_space=pltpu.VMEM)
    speed, place, change = pl.pallas_call(
        kernel,
        out_shape=(shape, shape, shape),
        in_specs=[pl.BlockSpec(memory_space=pl.ANY)] * len(args),
        out_specs=(vmem, vmem, vmem),
        scratch_shapes=[pltpu.VMEM(a.shape, a.dtype) for a in args]
        + [
            pltpu.VMEM((ROWS, elements), F32),
            pltpu.VMEM((ROWS, elements), F32),
            pltpu.VMEM((ROWS, elements), F32),
            pltpu.VMEM((RIM, elements), F32),
            pltpu.VMEM((RIM, elements), F32),
            pltpu.VMEM((PIECES * ROWS, 3 * ROWS), BF16),
            pltpu.VMEM((3 * RIM, 2 * ROWS), BF16),
            pltpu.VMEM((ROWS, 9 * RIM), BF16),
            pltpu.VMEM((ROWS, 3 * RIM), BF16),
            pltpu.VMEM((3 * ROWS, elements), BF16),
            pltpu.VMEM((3 * RIM, elements), F32),
            pltpu.VMEM((9 * RIM, elements), BF16),
            pltpu.VMEM((PIECES, elements), F32),
            pltpu.VMEM((1, elements), F32),
            pltpu.VMEM((3, 5, elements), F32),
            pltpu.VMEM((3, 2, elements), jnp.int32),
            pltpu.VMEM((5, elements), F32),
            pltpu.VMEM((MESSAGES, slots, LINES, LANES), F32),
            pltpu.VMEM((MESSAGES, slots, LINES, LANES), F32),
            pltpu.VMEM((MESSAGES, 2, RIM, LANES), F32),
            pltpu.VMEM((MESSAGES, 2, RIM, LANES), F32),
            pltpu.SemaphoreType.DMA((len(args),)),
            pltpu.SemaphoreType.DMA((MESSAGES,)),
            pltpu.SemaphoreType.DMA((MESSAGES,)),
            pltpu.SemaphoreType.DMA((MESSAGES, 2)),
            pltpu.SemaphoreType.DMA((MESSAGES, 2)),
        ],
        compiler_params=pltpu.CompilerParams(collective_id=0, has_side_effects=True),
    )(*args)
    return place + DT * change, speed + change


def solution(mesh):
    lanes = P(None, ("group", "sub"))
    state = P(None, None, ("group", "sub"))
    flat = P(("group", "sub"))
    return jax.shard_map(
        shards,
        mesh=mesh,
        in_specs=(state, state, lanes, flat, P(), P(), P(), lanes, lanes, lanes, lanes, flat, lanes),
        out_specs=(state, state),
        check_vma=False,
    )
```

```python
import jax
import jax.numpy as jnp
import numpy as np
from jax import lax
from jax.experimental import pallas as pl
from jax.experimental.pallas import tpu as pltpu
from jax.sharding import PartitionSpec as P

MESH = pl.DeviceIdType.MESH
F32 = jnp.float32
BF16 = jnp.bfloat16

DT = 0.25
NODES = 35
FN = 15
LANES = 128
ROWS = 112
RIM = 48
REST = NODES - FN
PIECES = 6
GROUPS = 4
SUBS = 32
SLOT = 8
ROUNDS = 3
MESSAGES = 2 * ROUNDS - 1
LINES = 3
NAMES = (
    "displacement", "velocity", "weights", "jacobian", "strain", "face_mass", "mass", "local_links", "local_geometry",
    "side_links", "side_geometry", "cross_links", "cross_geometry",
    "spread", "perm", "select", "place", "same", "face",
)


def row_of(c, n):
    return 16 * c + n if n < FN else RIM + REST * c + n - FN


def tables():
    points = [(a, b, c, 4 - a - b - c) for a in range(5) for b in range(5 - a) for c in range(5 - a - b)]
    faces = [[i for i, p in enumerate(points) if p[k] == 0] for k in range(4)]
    spread = np.zeros((ROWS, NODES), np.float32)
    perm = np.zeros((3 * NODES, ROWS), np.float32)
    select = np.zeros((4 * RIM, ROWS), np.float32)
    place = np.zeros((FN, 4 * RIM), np.float32)
    comp = np.full((ROWS,), -1, np.int64)
    for c in range(3):
        for n in range(NODES):
            spread[row_of(c, n), n] = 1.0
            perm[c * NODES + n, row_of(c, n)] = 1.0
            comp[row_of(c, n)] = c
        for k in range(4):
            for i, n in enumerate(faces[k]):
                select[k * RIM + 16 * c + i, row_of(c, n)] = 1.0
                place[i, k * RIM + 16 * c + i] = 1.0
    same = ((comp[:, None] == comp[None, :]) & (comp[:, None] >= 0)).astype(np.float32)
    block = np.arange(4 * RIM) // 16
    same_face = (block[:, None] == block[None, :]).astype(np.float32)
    return spread, perm.T.copy(), select, place, same, same_face


def one(a, b, dims=((1,), (0,))):
    return lax.dot_general(a, b, (dims, ((), ())), preferred_element_type=F32)


def dot(a, b, dims=((1,), (0,))):
    a, b = halves(a), halves(b)
    return one(a[0], b[0], dims) + (one(a[0], b[1], dims) + one(a[1], b[0], dims))


def halves(x):
    high = x.astype(BF16)
    return high, (x - high.astype(F32)).astype(BF16)


def traction(j, u, rigid, soft):
    jn = u[0] * j[0] + u[1] * j[1] + u[2] * j[2]
    size = j[0] * j[0] + j[1] * j[1] + j[2] * j[2] + jn * jn
    e = soft * jnp.exp(size * -0.125)
    a = rigid + e
    b = e * jn
    return [a * j[c] + b * u[c] for c in range(3)]


def kernel(*refs):
    count = len(NAMES)
    hbm = refs[:count]
    ovp, ofp, oc = refs[count : count + 3]
    buffers = refs[count + 3 : 2 * count + 3]
    (
        f, v, fp, p, ch, amat, smat, lmat, zmat, fh, tr, th, wj, ratio, lc, li, zc,
        xs, xr, ns, nr, in_sem, xs_sem, xr_sem, ns_sem, nr_sem,
    ) = refs[2 * count + 3 :]
    (
        d_ref, v_ref, w_ref, jac_ref, s_ref, fm_ref, mi_ref, ll_ref, lg_ref, nl_ref, ng_ref, cl_ref, cg_ref,
        spread_ref, perm_ref, select_ref, place_ref, same_ref, face_ref,
    ) = buffers
    loads = [pltpu.make_async_copy(hbm[k], buffers[k], in_sem.at[k]) for k in range(count)]
    g = lax.axis_index("group")
    s = lax.axis_index("sub")
    elements = f.shape[1]
    up = lax.rem(s + 1, SUBS)
    down = lax.rem(s + SUBS - 1, SUBS)
    barrier = pltpu.get_barrier_semaphore()

    def greet(t, carry):
        for b in range(GROUPS - 1):
            pl.semaphore_signal(
                barrier, inc=1, device_id=(lax.rem(g + 1 + b, GROUPS), t), device_id_type=MESH
            )
        return carry

    lax.fori_loop(0, SUBS, greet, 0, unroll=4)
    for t in (up, down):
        pl.semaphore_signal(barrier, inc=1, device_id=(g, t), device_id_type=MESH)
    first = (NAMES.index("displacement"), NAMES.index("jacobian"))
    for k in first:
        loads[k].start()
    for k in range(count):
        if k not in first:
            loads[k].start()

    def fill(source, target):
        for c in range(3):
            target[16 * c : 16 * c + FN, :] = source[c, 0:FN, :]
            target[16 * c + FN : 16 * c + FN + 1, :] = jnp.zeros((1, elements), F32)
            target[RIM + REST * c : RIM + REST * (c + 1), :] = source[c, FN:NODES, :]
        target[RIM + 3 * REST :, :] = jnp.zeros((ROWS - RIM - 3 * REST, elements), F32)

    for k in first:
        loads[k].wait()
    jac = jac_ref[...].reshape(1, elements)
    inv = 1.0 / jac
    fill(d_ref, f)
    f[FN : FN + 1, :] = inv

    def cross_copy(turn, b, t):
        return pltpu.make_async_remote_copy(
            src_ref=xs.at[turn, b * SUBS + t],
            dst_ref=xr.at[turn, (GROUPS - 2 - b) * SUBS + s],
            send_sem=xs_sem.at[turn],
            recv_sem=xr_sem.at[turn],
            device_id=(lax.rem(g + 1 + b, GROUPS), t),
            device_id_type=MESH,
        )

    def side_copy(turn, side):
        return pltpu.make_async_remote_copy(
            src_ref=ns.at[turn, side],
            dst_ref=nr.at[turn, 1 - side],
            send_sem=ns_sem.at[turn, side],
            recv_sem=nr_sem.at[turn, 1 - side],
            device_id=(g, down if side else up),
            device_id_type=MESH,
        )

    per = LANES // SLOT
    slot = lax.rem(lax.broadcasted_iota(jnp.int32, (8, LANES), 1), SLOT)

    def shift(x, by):
        return pltpu.roll(x, by % LANES, 1) if by % LANES else x

    def pack(turn, source):
        for block in range((GROUPS - 1) * SUBS // per):
            lanes = pl.ds((2 + block) * LANES, LANES)
            x = [source[8 * k : 8 * k + 8, lanes] for k in range(6)]
            tile = x + [shift(x[k], -3) for k in range(6)]
            for k in range(4):
                parts = []
                for r in range(3):
                    i = 4 * r + k
                    parts.append(shift(x[i % 6], r - (6 + i // 6)))
                tile.append(jnp.where(slot == 0, parts[0], jnp.where(slot == 1, parts[1], parts[2])))
            turned = jnp.concatenate(tile, axis=0).T.reshape(per, SLOT, LANES)
            xs[turn, block * per : (block + 1) * per, :, :] = turned[:, 0:LINES, :]
        for side in range(2):
            ns[turn, side, :, :] = source[0:RIM, pl.ds(side * LANES, LANES)]

    def send(turn):
        def go(k, carry):
            t = lax.rem(s + k, SUBS)
            for b in range(GROUPS - 1):
                cross_copy(turn, b, t).start()
            return carry

        lax.fori_loop(0, SUBS, go, 0, unroll=4)
        for side in range(2):
            side_copy(turn, side).start()

    def receive(turn, target):
        for side in range(2):
            side_copy(turn, 1 - side).wait_recv()
            target[:, pl.ds(side * LANES, LANES)] = nr[turn, side, :, :]
        pltpu.make_async_copy(xr.at[turn], xr.at[turn], xr_sem.at[turn]).wait()
        for block in range((GROUPS - 1) * SUBS // per):
            lanes = pl.ds((2 + block) * LANES, LANES)
            rows = xr[turn, block * per : (block + 1) * per, :, :]
            rows = jnp.concatenate([rows, jnp.zeros((per, SLOT - LINES, LANES), F32)], axis=1)
            tile = rows.reshape(LANES, LANES).T
            for k in range(6):
                x = tile[8 * k : 8 * k + 8, :]
                y = shift(tile[RIM + 8 * k : RIM + 8 * k + 8, :], 3)
                late = []
                for q in range(2):
                    i = 6 * q + k
                    at = 2 * RIM + 8 * (i % 4)
                    late.append(shift(tile[at : at + 8, :], 6 + q - i // 4))
                y = jnp.where(slot < 6, y, jnp.where(slot == 6, late[0], late[1]))
                target[8 * k : 8 * k + 8, lanes] = jnp.where(slot < 3, x, y)

    def empty(source, target):
        for c in range(3):
            target[c, 0:FN, :] = source[16 * c : 16 * c + FN, :]
            target[c, FN:NODES, :] = source[RIM + REST * c : RIM + REST * (c + 1), :]

    pack(0, f)

    for k in range(count):
        if k not in first:
            loads[k].wait()
    fill(v_ref, v)

    wj[...] = w_ref[...] * (inv * -DT)
    for q in range(3):
        part = pl.ds(q * elements, elements)
        state = ll_ref[1:2, part]
        scale = lg_ref[3:4, part] * (inv * DT)
        lc[q, 0:3, :] = lg_ref[0:3, part]
        lc[q, 3:4, :] = jnp.where(state == 0, scale, 0.0)
        lc[q, 4:5, :] = jnp.where(state == 1, 0.5 * scale, 0.0)
        partner = ll_ref[0:1, part]
        li[q, 0:1, :] = lax.rem(partner, LANES)
        li[q, 1:2, :] = lax.div(partner, LANES)
    cross = elements - 2 * LANES
    spots = (
        (0, LANES, ng_ref[0:4, :], nl_ref[0:1, :]),
        (LANES, LANES, ng_ref[4:8, :], nl_ref[1:2, :]),
        (2 * LANES, cross, cg_ref[...], cl_ref[...].reshape(1, cross)),
    )
    for at, size, geometry, state in spots:
        lanes = pl.ds(at, size)
        scale = geometry[3:4, :] * (inv[:, at : at + size] * DT)
        zc[0:3, lanes] = geometry[0:3, :]
        zc[3:4, lanes] = jnp.where(state == 0, scale, 0.0)
        zc[4:5, lanes] = jnp.where(state == 1, 0.5 * scale, 0.0)

    spread = spread_ref[...]
    mass = dot(dot(spread, mi_ref[...]), spread, ((1,), (1,))) * same_ref[...]
    flip = perm_ref[...].astype(BF16)
    strain = halves(s_ref[...])
    turned = one(flip, strain[0]) + one(flip, strain[1])
    left = [one(x, flip).astype(BF16) for x in halves(mass)]
    scaled = one(left[0], strain[0]) + (one(left[0], strain[1]) + one(left[1], strain[0]))
    for m in range(PIECES):
        columns = slice(m * 3 * NODES, (m + 1) * 3 * NODES)
        high, low = halves(dot(scaled[:, columns], turned[:, columns], ((1,), (1,))))
        rows = slice(m * ROWS, (m + 1) * ROWS)
        amat[rows, 0:ROWS] = high
        amat[rows, ROWS : 2 * ROWS] = high
        amat[rows, 2 * ROWS : 3 * ROWS] = low
    place = place_ref[...]
    face = dot(dot(place, fm_ref[...], ((0,), (0,))), place) * face_ref[...]
    lift = dot(mass, dot(select_ref[...], face, ((0,), (0,))))
    high, low = halves(lift)
    zmat[:, 0:RIM] = high[:, 0:RIM]
    zmat[:, RIM : 2 * RIM] = high[:, 0:RIM]
    zmat[:, 2 * RIM : 3 * RIM] = low[:, 0:RIM]
    lmat[:, 0 : 3 * RIM] = high[:, RIM:]
    lmat[:, 3 * RIM : 6 * RIM] = high[:, RIM:]
    lmat[:, 6 * RIM : 9 * RIM] = low[:, RIM:]
    chosen = select_ref[RIM:, :].astype(BF16)
    smat[:, 0:ROWS] = chosen
    smat[:, ROWS : 2 * ROWS] = chosen

    def local(width=2 * LANES):
        for at in range(0, elements, width):
            lanes = pl.ds(at, width)
            high, low = halves(f[:, lanes])
            fh[0:ROWS, lanes] = high
            fh[ROWS : 2 * ROWS, lanes] = low
            fh[2 * ROWS :, lanes] = high
            tr[:, lanes] = jnp.dot(smat[...], fh[0 : 2 * ROWS, lanes], preferred_element_type=F32)
        for at in range(0, elements, width):
            lanes = pl.ds(at, width)
            product = jnp.dot(amat[...], fh[:, lanes], preferred_element_type=F32)
            change = wj[0:1, lanes] * product[0:ROWS, :]
            for m in range(1, PIECES):
                change = change + wj[m : m + 1, lanes] * product[m * ROWS : (m + 1) * ROWS, :]
            v[:, lanes] = v[:, lanes] + change
            for block in range(at, at + width, LANES):
                pull(block)
        for at in range(0, elements, width):
            lanes = pl.ds(at, width)
            speed = v[:, lanes] + jnp.dot(lmat[...], th[:, lanes], preferred_element_type=F32)
            v[:, lanes] = speed
            fp[:, lanes] = f[:, lanes] + DT * speed

    def pull(block):
        here = pl.ds(block, LANES)
        for q in range(3):
            index = jnp.broadcast_to(li[q, 0:1, here], (16, LANES))
            origin = jnp.broadcast_to(li[q, 1:2, here], (16, LANES))
            jump = []
            for c in range(3):
                found = [
                    jnp.take_along_axis(
                        tr[r * RIM + 16 * c : r * RIM + 16 * (c + 1), here], index, axis=1, mode="promise_in_bounds"
                    )
                    for r in range(3)
                ]
                paired = jnp.where(origin == 0, found[0], jnp.where(origin == 1, found[1], found[2]))
                jump.append(paired - tr[q * RIM + 16 * c : q * RIM + 16 * (c + 1), here])
            parts = traction(
                jump, [lc[q, c : c + 1, here] for c in range(3)], lc[q, 3:4, here], lc[q, 4:5, here]
            )
            for c in range(3):
                high, low = halves(parts[c])
                at = q * RIM + 16 * c
                th[at : at + 16, here] = high
                th[3 * RIM + at : 3 * RIM + at + 16, here] = low
                th[6 * RIM + at : 6 * RIM + at + 16, here] = high

    def rim(keep, last=False, width=2 * LANES):
        for at in range(0, elements, width):
            lanes = pl.ds(at, width)
            jump = p[:, lanes] - f[0:RIM, lanes]
            pulled = jnp.concatenate(
                traction(
                    [jump[16 * c : 16 * (c + 1), :] for c in range(3)],
                    [zc[c : c + 1, lanes] for c in range(3)],
                    zc[3:4, lanes],
                    zc[4:5, lanes],
                ),
                axis=0,
            )
            high, low = halves(pulled)
            change = jnp.dot(
                zmat[...], jnp.concatenate([high, low, high], axis=0), preferred_element_type=F32
            )
            if last:
                f[:, lanes] = change
                continue
            v[:, lanes] = v[:, lanes] + change
            f[:, lanes] = fp[:, lanes] + DT * change
            if keep:
                ch[:, lanes] = change[0:RIM, :]

    def pair(turn, carry):
        local()
        pack(2 * turn + 1, fp)
        send(2 * turn + 1)
        receive(2 * turn, p)
        ratio[...] = p[FN : FN + 1, :] * (jac_ref[...].reshape(1, elements) * -DT)
        rim(True)
        local()
        receive(2 * turn + 1, p)
        for at in range(0, elements, 2 * LANES):
            lanes = pl.ds(at, 2 * LANES)
            p[:, lanes] = p[:, lanes] + ratio[0:1, lanes] * ch[:, lanes]
        rim(False)
        pack(2 * turn + 2, f)
        send(2 * turn + 2)
        return carry

    pl.semaphore_wait(barrier, (GROUPS - 1) * SUBS + 2)
    send(0)

    lax.fori_loop(0, ROUNDS - 1, pair, 0)
    local()
    empty(v, ovp)
    empty(fp, ofp)
    receive(2 * ROUNDS - 2, p)
    rim(False, True)
    empty(f, oc)
    for turn in range(MESSAGES):
        pltpu.make_async_copy(xs.at[turn], xs.at[turn], xs_sem.at[turn]).wait()
        for side in range(2):
            side_copy(turn, side).wait_send()


def shards(*args):
    elements = args[0].shape[2]
    shape = jax.ShapeDtypeStruct(args[0].shape, F32)
    args = args[:4] + (args[4].T,) + args[5:] + tuple(jnp.asarray(t) for t in tables())
    slots = (GROUPS - 1) * SUBS
    vmem = pl.BlockSpec(memory_space=pltpu.VMEM)
    speed, place, change = pl.pallas_call(
        kernel,
        out_shape=(pltpu.VMEM(shape.shape, F32),) * 3,
        in_specs=[pl.BlockSpec(memory_space=pl.ANY)] * len(args),
        out_specs=(vmem, vmem, vmem),
        scratch_shapes=[pltpu.VMEM(a.shape, a.dtype) for a in args]
        + [
            pltpu.VMEM((ROWS, elements), F32),
            pltpu.VMEM((ROWS, elements), F32),
            pltpu.VMEM((ROWS, elements), F32),
            pltpu.VMEM((RIM, elements), F32),
            pltpu.VMEM((RIM, elements), F32),
            pltpu.VMEM((PIECES * ROWS, 3 * ROWS), BF16),
            pltpu.VMEM((3 * RIM, 2 * ROWS), BF16),
            pltpu.VMEM((ROWS, 9 * RIM), BF16),
            pltpu.VMEM((ROWS, 3 * RIM), BF16),
            pltpu.VMEM((3 * ROWS, elements), BF16),
            pltpu.VMEM((3 * RIM, elements), F32),
            pltpu.VMEM((9 * RIM, elements), BF16),
            pltpu.VMEM((PIECES, elements), F32),
            pltpu.VMEM((1, elements), F32),
            pltpu.VMEM((3, 5, elements), F32),
            pltpu.VMEM((3, 2, elements), jnp.int32),
            pltpu.VMEM((5, elements), F32),
            pltpu.VMEM((MESSAGES, slots, LINES, LANES), F32),
            pltpu.VMEM((MESSAGES, slots, LINES, LANES), F32),
            pltpu.VMEM((MESSAGES, 2, RIM, LANES), F32),
            pltpu.VMEM((MESSAGES, 2, RIM, LANES), F32),
            pltpu.SemaphoreType.DMA((len(args),)),
            pltpu.SemaphoreType.DMA((MESSAGES,)),
            pltpu.SemaphoreType.DMA((MESSAGES,)),
            pltpu.SemaphoreType.DMA((MESSAGES, 2)),
            pltpu.SemaphoreType.DMA((MESSAGES, 2)),
        ],
        compiler_params=pltpu.CompilerParams(collective_id=0, has_side_effects=True),
    )(*args)
    return place + DT * change, speed + change


def solution(mesh):
    lanes = P(None, ("group", "sub"))
    state = P(None, None, ("group", "sub"))
    flat = P(("group", "sub"))
    return jax.shard_map(
        shards,
        mesh=mesh,
        in_specs=(state, state, lanes, flat, P(), P(), P(), lanes, lanes, lanes, lanes, flat, lanes),
        out_specs=(state, state),
        check_vma=False,
    )
```

```python
import jax
import jax.numpy as jnp
import numpy as np
from jax import lax
from jax.experimental import pallas as pl
from jax.experimental.pallas import tpu as pltpu
from jax.sharding import PartitionSpec as P

MESH = pl.DeviceIdType.MESH
F32 = jnp.float32
BF16 = jnp.bfloat16

DT = 0.25
NODES = 35
FN = 15
LANES = 128
ROWS = 112
RIM = 48
REST = NODES - FN
PIECES = 6
GROUPS = 4
SUBS = 32
SLOT = 8
ROUNDS = 3
MESSAGES = 2 * ROUNDS - 1
LINES = 3
NAMES = (
    "displacement", "velocity", "weights", "jacobian", "strain", "face_mass", "mass", "local_links", "local_geometry",
    "side_links", "side_geometry", "cross_links", "cross_geometry",
    "spread", "perm", "select", "place", "same", "face",
)


def reach(k):
    return -sum(min(d, 4 - d) for d in (k // 8, k // 2 % 4))


def row_of(c, n):
    return 16 * c + n if n < FN else RIM + REST * c + n - FN


def tables():
    points = [(a, b, c, 4 - a - b - c) for a in range(5) for b in range(5 - a) for c in range(5 - a - b)]
    faces = [[i for i, p in enumerate(points) if p[k] == 0] for k in range(4)]
    spread = np.zeros((ROWS, NODES), np.float32)
    perm = np.zeros((3 * NODES, ROWS), np.float32)
    select = np.zeros((4 * RIM, ROWS), np.float32)
    place = np.zeros((FN, 4 * RIM), np.float32)
    comp = np.full((ROWS,), -1, np.int64)
    for c in range(3):
        for n in range(NODES):
            spread[row_of(c, n), n] = 1.0
            perm[c * NODES + n, row_of(c, n)] = 1.0
            comp[row_of(c, n)] = c
        for k in range(4):
            for i, n in enumerate(faces[k]):
                select[k * RIM + 16 * c + i, row_of(c, n)] = 1.0
                place[i, k * RIM + 16 * c + i] = 1.0
    same = ((comp[:, None] == comp[None, :]) & (comp[:, None] >= 0)).astype(np.float32)
    block = np.arange(4 * RIM) // 16
    same_face = (block[:, None] == block[None, :]).astype(np.float32)
    return spread, perm.T.copy(), select, place, same, same_face


def one(a, b, dims=((1,), (0,))):
    return lax.dot_general(a, b, (dims, ((), ())), preferred_element_type=F32)


def dot(a, b, dims=((1,), (0,))):
    a, b = halves(a), halves(b)
    return one(a[0], b[0], dims) + (one(a[0], b[1], dims) + one(a[1], b[0], dims))


def halves(x):
    high = x.astype(BF16)
    return high, (x - high.astype(F32)).astype(BF16)


def traction(j, u, rigid, soft):
    jn = u[0] * j[0] + u[1] * j[1] + u[2] * j[2]
    size = j[0] * j[0] + j[1] * j[1] + j[2] * j[2] + jn * jn
    e = soft * jnp.exp(size * -0.125)
    a = rigid + e
    b = e * jn
    return [a * j[c] + b * u[c] for c in range(3)]


def kernel(*refs):
    count = len(NAMES)
    hbm = refs[:count]
    ovp, ofp, oc = refs[count : count + 3]
    buffers = refs[count + 3 : 2 * count + 3]
    (
        f, v, fp, p, ch, amat, smat, lmat, zmat, fh, tr, th, wj, ratio, lc, li, zc,
        xs, xr, ns, nr, in_sem, xs_sem, xr_sem, ns_sem, nr_sem,
    ) = refs[2 * count + 3 :]
    (
        d_ref, v_ref, w_ref, jac_ref, s_ref, fm_ref, mi_ref, ll_ref, lg_ref, nl_ref, ng_ref, cl_ref, cg_ref,
        spread_ref, perm_ref, select_ref, place_ref, same_ref, face_ref,
    ) = buffers
    loads = [pltpu.make_async_copy(hbm[k], buffers[k], in_sem.at[k]) for k in range(count)]
    g = lax.axis_index("group")
    s = lax.axis_index("sub")
    elements = f.shape[1]
    up = lax.rem(s + 1, SUBS)
    down = lax.rem(s + SUBS - 1, SUBS)
    barrier = pltpu.get_barrier_semaphore()

    def greet(t, carry):
        for b in range(GROUPS - 1):
            pl.semaphore_signal(
                barrier, inc=1, device_id=(lax.rem(g + 1 + b, GROUPS), t), device_id_type=MESH
            )
        return carry

    lax.fori_loop(0, SUBS, greet, 0, unroll=4)
    for t in (up, down):
        pl.semaphore_signal(barrier, inc=1, device_id=(g, t), device_id_type=MESH)
    first = (NAMES.index("displacement"), NAMES.index("jacobian"))
    for k in first:
        loads[k].start()
    for k in range(count):
        if k not in first:
            loads[k].start()

    def fill(source, target):
        for c in range(3):
            target[16 * c : 16 * c + FN, :] = source[c, 0:FN, :]
            target[16 * c + FN : 16 * c + FN + 1, :] = jnp.zeros((1, elements), F32)
            target[RIM + REST * c : RIM + REST * (c + 1), :] = source[c, FN:NODES, :]
        target[RIM + 3 * REST :, :] = jnp.zeros((ROWS - RIM - 3 * REST, elements), F32)

    for k in first:
        loads[k].wait()
    jac = jac_ref[...].reshape(1, elements)
    inv = 1.0 / jac
    fill(d_ref, f)
    f[FN : FN + 1, :] = inv

    def cross_copy(turn, b, t):
        return pltpu.make_async_remote_copy(
            src_ref=xs.at[turn, b * SUBS + t],
            dst_ref=xr.at[turn, (GROUPS - 2 - b) * SUBS + s],
            send_sem=xs_sem.at[turn],
            recv_sem=xr_sem.at[turn],
            device_id=(lax.rem(g + 1 + b, GROUPS), t),
            device_id_type=MESH,
        )

    def side_copy(turn, side):
        return pltpu.make_async_remote_copy(
            src_ref=ns.at[turn, side],
            dst_ref=nr.at[turn, 1 - side],
            send_sem=ns_sem.at[turn, side],
            recv_sem=nr_sem.at[turn, 1 - side],
            device_id=(g, down if side else up),
            device_id_type=MESH,
        )

    per = LANES // SLOT
    slot = lax.rem(lax.broadcasted_iota(jnp.int32, (8, LANES), 1), SLOT)

    def shift(x, by):
        return pltpu.roll(x, by % LANES, 1) if by % LANES else x

    def pack(turn, source):
        for block in range((GROUPS - 1) * SUBS // per):
            lanes = pl.ds((2 + block) * LANES, LANES)
            x = [source[8 * k : 8 * k + 8, lanes] for k in range(6)]
            tile = x + [shift(x[k], -3) for k in range(6)]
            for k in range(4):
                parts = []
                for r in range(3):
                    i = 4 * r + k
                    parts.append(shift(x[i % 6], r - (6 + i // 6)))
                tile.append(jnp.where(slot == 0, parts[0], jnp.where(slot == 1, parts[1], parts[2])))
            turned = jnp.concatenate(tile, axis=0).T.reshape(per, SLOT, LANES)
            xs[turn, block * per : (block + 1) * per, :, :] = turned[:, 0:LINES, :]
        for side in range(2):
            ns[turn, side, :, :] = source[0:RIM, pl.ds(side * LANES, LANES)]

    def send(turn):
        for k in sorted(range(SUBS), key=reach):
            t = lax.rem(s + k, SUBS)
            for b in (1, 0, 2):
                cross_copy(turn, b, t).start()
        for side in range(2):
            side_copy(turn, side).start()

    def receive(turn, target):
        for side in range(2):
            side_copy(turn, 1 - side).wait_recv()
            target[:, pl.ds(side * LANES, LANES)] = nr[turn, side, :, :]
        pltpu.make_async_copy(xr.at[turn], xr.at[turn], xr_sem.at[turn]).wait()
        for block in range((GROUPS - 1) * SUBS // per):
            lanes = pl.ds((2 + block) * LANES, LANES)
            rows = xr[turn, block * per : (block + 1) * per, :, :]
            rows = jnp.concatenate([rows, jnp.zeros((per, SLOT - LINES, LANES), F32)], axis=1)
            tile = rows.reshape(LANES, LANES).T
            for k in range(6):
                x = tile[8 * k : 8 * k + 8, :]
                y = shift(tile[RIM + 8 * k : RIM + 8 * k + 8, :], 3)
                late = []
                for q in range(2):
                    i = 6 * q + k
                    at = 2 * RIM + 8 * (i % 4)
                    late.append(shift(tile[at : at + 8, :], 6 + q - i // 4))
                y = jnp.where(slot < 6, y, jnp.where(slot == 6, late[0], late[1]))
                target[8 * k : 8 * k + 8, lanes] = jnp.where(slot < 3, x, y)

    def empty(source, target):
        for c in range(3):
            target[c, 0:FN, :] = source[16 * c : 16 * c + FN, :]
            target[c, FN:NODES, :] = source[RIM + REST * c : RIM + REST * (c + 1), :]

    pack(0, f)

    for k in range(count):
        if k not in first:
            loads[k].wait()
    fill(v_ref, v)

    wj[...] = w_ref[...] * (inv * -DT)
    for q in range(3):
        part = pl.ds(q * elements, elements)
        state = ll_ref[1:2, part]
        scale = lg_ref[3:4, part] * (inv * DT)
        lc[q, 0:3, :] = lg_ref[0:3, part]
        lc[q, 3:4, :] = jnp.where(state == 0, scale, 0.0)
        lc[q, 4:5, :] = jnp.where(state == 1, 0.5 * scale, 0.0)
        partner = ll_ref[0:1, part]
        li[q, 0:1, :] = lax.rem(partner, LANES)
        li[q, 1:2, :] = lax.div(partner, LANES)
    cross = elements - 2 * LANES
    spots = (
        (0, LANES, ng_ref[0:4, :], nl_ref[0:1, :]),
        (LANES, LANES, ng_ref[4:8, :], nl_ref[1:2, :]),
        (2 * LANES, cross, cg_ref[...], cl_ref[...].reshape(1, cross)),
    )
    for at, size, geometry, state in spots:
        lanes = pl.ds(at, size)
        scale = geometry[3:4, :] * (inv[:, at : at + size] * DT)
        zc[0:3, lanes] = geometry[0:3, :]
        zc[3:4, lanes] = jnp.where(state == 0, scale, 0.0)
        zc[4:5, lanes] = jnp.where(state == 1, 0.5 * scale, 0.0)

    spread = spread_ref[...]
    mass = dot(dot(spread, mi_ref[...]), spread, ((1,), (1,))) * same_ref[...]
    flip = perm_ref[...].astype(BF16)
    strain = halves(s_ref[...])
    turned = one(flip, strain[0]) + one(flip, strain[1])
    left = [one(x, flip).astype(BF16) for x in halves(mass)]
    scaled = one(left[0], strain[0]) + (one(left[0], strain[1]) + one(left[1], strain[0]))
    for m in range(PIECES):
        columns = slice(m * 3 * NODES, (m + 1) * 3 * NODES)
        high, low = halves(dot(scaled[:, columns], turned[:, columns], ((1,), (1,))))
        rows = slice(m * ROWS, (m + 1) * ROWS)
        amat[rows, 0:ROWS] = high
        amat[rows, ROWS : 2 * ROWS] = high
        amat[rows, 2 * ROWS : 3 * ROWS] = low
    place = place_ref[...]
    face = dot(dot(place, fm_ref[...], ((0,), (0,))), place) * face_ref[...]
    lift = dot(mass, dot(select_ref[...], face, ((0,), (0,))))
    high, low = halves(lift)
    zmat[:, 0:RIM] = high[:, 0:RIM]
    zmat[:, RIM : 2 * RIM] = high[:, 0:RIM]
    zmat[:, 2 * RIM : 3 * RIM] = low[:, 0:RIM]
    lmat[:, 0 : 3 * RIM] = high[:, RIM:]
    lmat[:, 3 * RIM : 6 * RIM] = high[:, RIM:]
    lmat[:, 6 * RIM : 9 * RIM] = low[:, RIM:]
    chosen = select_ref[RIM:, :].astype(BF16)
    smat[:, 0:ROWS] = chosen
    smat[:, ROWS : 2 * ROWS] = chosen

    def local(width=2 * LANES):
        for at in range(0, elements, width):
            lanes = pl.ds(at, width)
            high, low = halves(f[:, lanes])
            fh[0:ROWS, lanes] = high
            fh[ROWS : 2 * ROWS, lanes] = low
            tr[:, lanes] = jnp.dot(smat[...], fh[0 : 2 * ROWS, lanes], preferred_element_type=F32)
        for at in range(0, elements, width):
            lanes = pl.ds(at, width)
            product = jnp.dot(
                amat[...], jnp.concatenate([fh[:, lanes], fh[0:ROWS, lanes]], axis=0), preferred_element_type=F32
            )
            change = wj[0:1, lanes] * product[0:ROWS, :]
            for m in range(1, PIECES):
                change = change + wj[m : m + 1, lanes] * product[m * ROWS : (m + 1) * ROWS, :]
            v[:, lanes] = v[:, lanes] + change
            for block in range(at, at + width, LANES):
                pull(block)
        for at in range(0, elements, width):
            lanes = pl.ds(at, width)
            speed = v[:, lanes] + jnp.dot(
                lmat[...], jnp.concatenate([th[:, lanes], th[0 : 3 * RIM, lanes]], axis=0), preferred_element_type=F32
            )
            v[:, lanes] = speed
            fp[:, lanes] = f[:, lanes] + DT * speed

    def pull(block):
        here = pl.ds(block, LANES)
        for q in range(3):
            index = jnp.broadcast_to(li[q, 0:1, here], (16, LANES))
            origin = jnp.broadcast_to(li[q, 1:2, here], (16, LANES))
            jump = []
            for c in range(3):
                found = [
                    jnp.take_along_axis(
                        tr[r * RIM + 16 * c : r * RIM + 16 * (c + 1), here], index, axis=1, mode="promise_in_bounds"
                    )
                    for r in range(3)
                ]
                paired = jnp.where(origin == 0, found[0], jnp.where(origin == 1, found[1], found[2]))
                jump.append(paired - tr[q * RIM + 16 * c : q * RIM + 16 * (c + 1), here])
            parts = traction(
                jump, [lc[q, c : c + 1, here] for c in range(3)], lc[q, 3:4, here], lc[q, 4:5, here]
            )
            for c in range(3):
                high, low = halves(parts[c])
                at = q * RIM + 16 * c
                th[at : at + 16, here] = high
                th[3 * RIM + at : 3 * RIM + at + 16, here] = low

    def rim(keep, last=False, width=2 * LANES):
        for at in range(0, elements, width):
            lanes = pl.ds(at, width)
            jump = p[:, lanes] - f[0:RIM, lanes]
            pulled = jnp.concatenate(
                traction(
                    [jump[16 * c : 16 * (c + 1), :] for c in range(3)],
                    [zc[c : c + 1, lanes] for c in range(3)],
                    zc[3:4, lanes],
                    zc[4:5, lanes],
                ),
                axis=0,
            )
            high, low = halves(pulled)
            change = jnp.dot(
                zmat[...], jnp.concatenate([high, low, high], axis=0), preferred_element_type=F32
            )
            if last:
                f[:, lanes] = change
                continue
            v[:, lanes] = v[:, lanes] + change
            f[:, lanes] = fp[:, lanes] + DT * change
            if keep:
                ch[:, lanes] = change[0:RIM, :]

    def pair(turn, carry):
        local()
        pack(2 * turn + 1, fp)
        send(2 * turn + 1)
        receive(2 * turn, p)
        ratio[...] = p[FN : FN + 1, :] * (jac_ref[...].reshape(1, elements) * -DT)
        rim(True)
        local()
        receive(2 * turn + 1, p)
        for at in range(0, elements, 2 * LANES):
            lanes = pl.ds(at, 2 * LANES)
            p[:, lanes] = p[:, lanes] + ratio[0:1, lanes] * ch[:, lanes]
        rim(False)
        pack(2 * turn + 2, f)
        send(2 * turn + 2)
        return carry

    pl.semaphore_wait(barrier, (GROUPS - 1) * SUBS + 2)
    send(0)

    lax.fori_loop(0, ROUNDS - 1, pair, 0)
    local()
    empty(v, ovp)
    empty(fp, ofp)
    receive(2 * ROUNDS - 2, p)
    rim(False, True)
    empty(f, oc)
    for turn in range(MESSAGES):
        pltpu.make_async_copy(xs.at[turn], xs.at[turn], xs_sem.at[turn]).wait()
        for side in range(2):
            side_copy(turn, side).wait_send()


def shards(*args):
    elements = args[0].shape[2]
    shape = jax.ShapeDtypeStruct(args[0].shape, F32)
    args = args[:4] + (args[4].T,) + args[5:] + tuple(jnp.asarray(t) for t in tables())
    slots = (GROUPS - 1) * SUBS
    vmem = pl.BlockSpec(memory_space=pltpu.VMEM)
    speed, place, change = pl.pallas_call(
        kernel,
        out_shape=(pltpu.VMEM(shape.shape, F32),) * 3,
        in_specs=[pl.BlockSpec(memory_space=pl.ANY)] * len(args),
        out_specs=(vmem, vmem, vmem),
        scratch_shapes=[pltpu.VMEM(a.shape, a.dtype) for a in args]
        + [
            pltpu.VMEM((ROWS, elements), F32),
            pltpu.VMEM((ROWS, elements), F32),
            pltpu.VMEM((ROWS, elements), F32),
            pltpu.VMEM((RIM, elements), F32),
            pltpu.VMEM((RIM, elements), F32),
            pltpu.VMEM((PIECES * ROWS, 3 * ROWS), BF16),
            pltpu.VMEM((3 * RIM, 2 * ROWS), BF16),
            pltpu.VMEM((ROWS, 9 * RIM), BF16),
            pltpu.VMEM((ROWS, 3 * RIM), BF16),
            pltpu.VMEM((2 * ROWS, elements), BF16),
            pltpu.VMEM((3 * RIM, elements), F32),
            pltpu.VMEM((6 * RIM, elements), BF16),
            pltpu.VMEM((PIECES, elements), F32),
            pltpu.VMEM((1, elements), F32),
            pltpu.VMEM((3, 5, elements), F32),
            pltpu.VMEM((3, 2, elements), jnp.int32),
            pltpu.VMEM((5, elements), F32),
            pltpu.VMEM((MESSAGES, slots, LINES, LANES), F32),
            pltpu.VMEM((MESSAGES, slots, LINES, LANES), F32),
            pltpu.VMEM((MESSAGES, 2, RIM, LANES), F32),
            pltpu.VMEM((MESSAGES, 2, RIM, LANES), F32),
            pltpu.SemaphoreType.DMA((len(args),)),
            pltpu.SemaphoreType.DMA((MESSAGES,)),
            pltpu.SemaphoreType.DMA((MESSAGES,)),
            pltpu.SemaphoreType.DMA((MESSAGES, 2)),
            pltpu.SemaphoreType.DMA((MESSAGES, 2)),
        ],
        compiler_params=pltpu.CompilerParams(collective_id=0, has_side_effects=True),
    )(*args)
    return place + DT * change, speed + change


def solution(mesh):
    lanes = P(None, ("group", "sub"))
    state = P(None, None, ("group", "sub"))
    flat = P(("group", "sub"))
    return jax.shard_map(
        shards,
        mesh=mesh,
        in_specs=(state, state, lanes, flat, P(), P(), P(), lanes, lanes, lanes, lanes, flat, lanes),
        out_specs=(state, state),
        check_vma=False,
    )
```

```python
import jax
import jax.numpy as jnp
import numpy as np
from jax import lax
from jax.experimental import pallas as pl
from jax.experimental.pallas import tpu as pltpu
from jax.sharding import PartitionSpec as P

MESH = pl.DeviceIdType.MESH
F32 = jnp.float32
BF16 = jnp.bfloat16

DT = 0.25
NODES = 35
FN = 15
LANES = 128
ROWS = 112
RIM = 48
REST = NODES - FN
PIECES = 6
GROUPS = 4
SUBS = 32
SLOT = 8
ROUNDS = 3
MESSAGES = 2 * ROUNDS - 1
LINES = 3
NAMES = (
    "displacement", "velocity", "weights", "jacobian", "strain", "face_mass", "mass", "local_links", "local_geometry",
    "side_links", "side_geometry", "cross_links", "cross_geometry",
    "spread", "perm", "select", "place", "same", "face",
)


def reach(k):
    return -sum(min(d, 4 - d) for d in (k // 8, k // 2 % 4))


def row_of(c, n):
    return 16 * c + n if n < FN else RIM + REST * c + n - FN


def tables():
    points = [(a, b, c, 4 - a - b - c) for a in range(5) for b in range(5 - a) for c in range(5 - a - b)]
    faces = [[i for i, p in enumerate(points) if p[k] == 0] for k in range(4)]
    spread = np.zeros((ROWS, NODES), np.float32)
    perm = np.zeros((3 * NODES, ROWS), np.float32)
    select = np.zeros((4 * RIM, ROWS), np.float32)
    place = np.zeros((FN, 4 * RIM), np.float32)
    comp = np.full((ROWS,), -1, np.int64)
    for c in range(3):
        for n in range(NODES):
            spread[row_of(c, n), n] = 1.0
            perm[c * NODES + n, row_of(c, n)] = 1.0
            comp[row_of(c, n)] = c
        for k in range(4):
            for i, n in enumerate(faces[k]):
                select[k * RIM + 16 * c + i, row_of(c, n)] = 1.0
                place[i, k * RIM + 16 * c + i] = 1.0
    same = ((comp[:, None] == comp[None, :]) & (comp[:, None] >= 0)).astype(np.float32)
    block = np.arange(4 * RIM) // 16
    same_face = (block[:, None] == block[None, :]).astype(np.float32)
    return spread, perm.T.copy(), select, place, same, same_face


def one(a, b, dims=((1,), (0,))):
    return lax.dot_general(a, b, (dims, ((), ())), preferred_element_type=F32)


def dot(a, b, dims=((1,), (0,))):
    a, b = halves(a), halves(b)
    return one(a[0], b[0], dims) + (one(a[0], b[1], dims) + one(a[1], b[0], dims))


def halves(x):
    high = x.astype(BF16)
    return high, (x - high.astype(F32)).astype(BF16)


def traction(j, u, rigid, soft):
    jn = u[0] * j[0] + u[1] * j[1] + u[2] * j[2]
    size = j[0] * j[0] + j[1] * j[1] + j[2] * j[2] + jn * jn
    e = soft * jnp.exp(size * -0.125)
    a = rigid + e
    b = e * jn
    return [a * j[c] + b * u[c] for c in range(3)]


def kernel(*refs):
    count = len(NAMES)
    hbm = refs[:count]
    ovp, ofp, oc = refs[count : count + 3]
    buffers = refs[count + 3 : 2 * count + 3]
    (
        f, v, fp, p, ch, amat, smat, lmat, zmat, fh, tr, th, wj, ratio, lc, li, zc,
        xs, xr, ns, nr, in_sem, xs_sem, xr_sem, ns_sem, nr_sem,
    ) = refs[2 * count + 3 :]
    (
        d_ref, v_ref, w_ref, jac_ref, s_ref, fm_ref, mi_ref, ll_ref, lg_ref, nl_ref, ng_ref, cl_ref, cg_ref,
        spread_ref, perm_ref, select_ref, place_ref, same_ref, face_ref,
    ) = buffers
    loads = [pltpu.make_async_copy(hbm[k], buffers[k], in_sem.at[k]) for k in range(count)]
    g = lax.axis_index("group")
    s = lax.axis_index("sub")
    elements = f.shape[1]
    up = lax.rem(s + 1, SUBS)
    down = lax.rem(s + SUBS - 1, SUBS)
    barrier = pltpu.get_barrier_semaphore()

    for k in sorted(range(SUBS), key=reach):
        for b in (1, 0, 2):
            pl.semaphore_signal(
                barrier, inc=1, device_id=(lax.rem(g + 1 + b, GROUPS), lax.rem(s + k, SUBS)), device_id_type=MESH
            )
    for t in (up, down):
        pl.semaphore_signal(barrier, inc=1, device_id=(g, t), device_id_type=MESH)
    first = (NAMES.index("displacement"), NAMES.index("jacobian"))
    for k in first:
        loads[k].start()
    for k in range(count):
        if k not in first:
            loads[k].start()

    def fill(source, target):
        for c in range(3):
            target[16 * c : 16 * c + FN, :] = source[c, 0:FN, :]
            target[16 * c + FN : 16 * c + FN + 1, :] = jnp.zeros((1, elements), F32)
            target[RIM + REST * c : RIM + REST * (c + 1), :] = source[c, FN:NODES, :]
        target[RIM + 3 * REST :, :] = jnp.zeros((ROWS - RIM - 3 * REST, elements), F32)

    for k in first:
        loads[k].wait()
    jac = jac_ref[...].reshape(1, elements)
    inv = 1.0 / jac
    fill(d_ref, f)
    f[FN : FN + 1, :] = inv

    def cross_copy(turn, b, t):
        return pltpu.make_async_remote_copy(
            src_ref=xs.at[turn, b * SUBS + t],
            dst_ref=xr.at[turn, (GROUPS - 2 - b) * SUBS + s],
            send_sem=xs_sem.at[turn],
            recv_sem=xr_sem.at[turn],
            device_id=(lax.rem(g + 1 + b, GROUPS), t),
            device_id_type=MESH,
        )

    def side_copy(turn, side):
        return pltpu.make_async_remote_copy(
            src_ref=ns.at[turn, side],
            dst_ref=nr.at[turn, 1 - side],
            send_sem=ns_sem.at[turn, side],
            recv_sem=nr_sem.at[turn, 1 - side],
            device_id=(g, down if side else up),
            device_id_type=MESH,
        )

    per = LANES // SLOT
    slot = lax.rem(lax.broadcasted_iota(jnp.int32, (8, LANES), 1), SLOT)

    def shift(x, by):
        return pltpu.roll(x, by % LANES, 1) if by % LANES else x

    def pack(turn, source):
        for block in range((GROUPS - 1) * SUBS // per):
            lanes = pl.ds((2 + block) * LANES, LANES)
            x = [source[8 * k : 8 * k + 8, lanes] for k in range(6)]
            tile = x + [shift(x[k], -3) for k in range(6)]
            for k in range(4):
                parts = []
                for r in range(3):
                    i = 4 * r + k
                    parts.append(shift(x[i % 6], r - (6 + i // 6)))
                tile.append(jnp.where(slot == 0, parts[0], jnp.where(slot == 1, parts[1], parts[2])))
            turned = jnp.concatenate(tile, axis=0).T.reshape(per, SLOT, LANES)
            xs[turn, block * per : (block + 1) * per, :, :] = turned[:, 0:LINES, :]
        for side in range(2):
            ns[turn, side, :, :] = source[0:RIM, pl.ds(side * LANES, LANES)]

    def send(turn):
        for k in sorted(range(SUBS), key=reach):
            t = lax.rem(s + k, SUBS)
            for b in (1, 0, 2):
                cross_copy(turn, b, t).start()
        for side in range(2):
            side_copy(turn, side).start()

    def receive(turn, target):
        for side in range(2):
            side_copy(turn, 1 - side).wait_recv()
            target[:, pl.ds(side * LANES, LANES)] = nr[turn, side, :, :]
        pltpu.make_async_copy(xr.at[turn], xr.at[turn], xr_sem.at[turn]).wait()
        for block in range((GROUPS - 1) * SUBS // per):
            lanes = pl.ds((2 + block) * LANES, LANES)
            rows = xr[turn, block * per : (block + 1) * per, :, :]
            rows = jnp.concatenate([rows, jnp.zeros((per, SLOT - LINES, LANES), F32)], axis=1)
            tile = rows.reshape(LANES, LANES).T
            for k in range(6):
                x = tile[8 * k : 8 * k + 8, :]
                y = shift(tile[RIM + 8 * k : RIM + 8 * k + 8, :], 3)
                late = []
                for q in range(2):
                    i = 6 * q + k
                    at = 2 * RIM + 8 * (i % 4)
                    late.append(shift(tile[at : at + 8, :], 6 + q - i // 4))
                y = jnp.where(slot < 6, y, jnp.where(slot == 6, late[0], late[1]))
                target[8 * k : 8 * k + 8, lanes] = jnp.where(slot < 3, x, y)

    def empty(source, target):
        for c in range(3):
            target[c, 0:FN, :] = source[16 * c : 16 * c + FN, :]
            target[c, FN:NODES, :] = source[RIM + REST * c : RIM + REST * (c + 1), :]

    pack(0, f)

    for k in range(count):
        if k not in first:
            loads[k].wait()
    fill(v_ref, v)

    wj[...] = w_ref[...] * (inv * -DT)
    for q in range(3):
        part = pl.ds(q * elements, elements)
        state = ll_ref[1:2, part]
        scale = lg_ref[3:4, part] * (inv * DT)
        lc[q, 0:3, :] = lg_ref[0:3, part]
        lc[q, 3:4, :] = jnp.where(state == 0, scale, 0.0)
        lc[q, 4:5, :] = jnp.where(state == 1, 0.5 * scale, 0.0)
        partner = ll_ref[0:1, part]
        li[q, 0:1, :] = lax.rem(partner, LANES)
        li[q, 1:2, :] = lax.div(partner, LANES)
    cross = elements - 2 * LANES
    spots = (
        (0, LANES, ng_ref[0:4, :], nl_ref[0:1, :]),
        (LANES, LANES, ng_ref[4:8, :], nl_ref[1:2, :]),
        (2 * LANES, cross, cg_ref[...], cl_ref[...].reshape(1, cross)),
    )
    for at, size, geometry, state in spots:
        lanes = pl.ds(at, size)
        scale = geometry[3:4, :] * (inv[:, at : at + size] * DT)
        zc[0:3, lanes] = geometry[0:3, :]
        zc[3:4, lanes] = jnp.where(state == 0, scale, 0.0)
        zc[4:5, lanes] = jnp.where(state == 1, 0.5 * scale, 0.0)

    spread = spread_ref[...]
    mass = dot(dot(spread, mi_ref[...]), spread, ((1,), (1,))) * same_ref[...]
    flip = perm_ref[...].astype(BF16)
    strain = halves(s_ref[...])
    turned = one(flip, strain[0]) + one(flip, strain[1])
    left = [one(x, flip).astype(BF16) for x in halves(mass)]
    scaled = one(left[0], strain[0]) + (one(left[0], strain[1]) + one(left[1], strain[0]))
    for m in range(PIECES):
        columns = slice(m * 3 * NODES, (m + 1) * 3 * NODES)
        high, low = halves(dot(scaled[:, columns], turned[:, columns], ((1,), (1,))))
        rows = slice(m * ROWS, (m + 1) * ROWS)
        amat[rows, 0:ROWS] = high
        amat[rows, ROWS : 2 * ROWS] = high
        amat[rows, 2 * ROWS : 3 * ROWS] = low
    place = place_ref[...]
    face = dot(dot(place, fm_ref[...], ((0,), (0,))), place) * face_ref[...]
    lift = dot(mass, dot(select_ref[...], face, ((0,), (0,))))
    high, low = halves(lift)
    zmat[:, 0:RIM] = high[:, 0:RIM]
    zmat[:, RIM : 2 * RIM] = high[:, 0:RIM]
    zmat[:, 2 * RIM : 3 * RIM] = low[:, 0:RIM]
    lmat[:, 0 : 3 * RIM] = high[:, RIM:]
    lmat[:, 3 * RIM : 6 * RIM] = high[:, RIM:]
    lmat[:, 6 * RIM : 9 * RIM] = low[:, RIM:]
    chosen = select_ref[RIM:, :].astype(BF16)
    smat[:, 0:ROWS] = chosen
    smat[:, ROWS : 2 * ROWS] = chosen

    def local(width=2 * LANES):
        for at in range(0, elements, width):
            lanes = pl.ds(at, width)
            high, low = halves(f[:, lanes])
            fh[0:ROWS, lanes] = high
            fh[ROWS : 2 * ROWS, lanes] = low
            tr[:, lanes] = jnp.dot(smat[...], fh[0 : 2 * ROWS, lanes], preferred_element_type=F32)
        for at in range(0, elements, width):
            lanes = pl.ds(at, width)
            product = jnp.dot(
                amat[...], jnp.concatenate([fh[:, lanes], fh[0:ROWS, lanes]], axis=0), preferred_element_type=F32
            )
            change = wj[0:1, lanes] * product[0:ROWS, :]
            for m in range(1, PIECES):
                change = change + wj[m : m + 1, lanes] * product[m * ROWS : (m + 1) * ROWS, :]
            v[:, lanes] = v[:, lanes] + change
            for block in range(at, at + width, LANES):
                pull(block)
        for at in range(0, elements, width):
            lanes = pl.ds(at, width)
            speed = v[:, lanes] + jnp.dot(
                lmat[...], jnp.concatenate([th[:, lanes], th[0 : 3 * RIM, lanes]], axis=0), preferred_element_type=F32
            )
            v[:, lanes] = speed
            fp[:, lanes] = f[:, lanes] + DT * speed

    def pull(block):
        here = pl.ds(block, LANES)
        for q in range(3):
            index = jnp.broadcast_to(li[q, 0:1, here], (16, LANES))
            origin = jnp.broadcast_to(li[q, 1:2, here], (16, LANES))
            jump = []
            for c in range(3):
                found = [
                    jnp.take_along_axis(
                        tr[r * RIM + 16 * c : r * RIM + 16 * (c + 1), here], index, axis=1, mode="promise_in_bounds"
                    )
                    for r in range(3)
                ]
                paired = jnp.where(origin == 0, found[0], jnp.where(origin == 1, found[1], found[2]))
                jump.append(paired - tr[q * RIM + 16 * c : q * RIM + 16 * (c + 1), here])
            parts = traction(
                jump, [lc[q, c : c + 1, here] for c in range(3)], lc[q, 3:4, here], lc[q, 4:5, here]
            )
            for c in range(3):
                high, low = halves(parts[c])
                at = q * RIM + 16 * c
                th[at : at + 16, here] = high
                th[3 * RIM + at : 3 * RIM + at + 16, here] = low

    def rim(keep, last=False, width=2 * LANES):
        for at in range(0, elements, width):
            lanes = pl.ds(at, width)
            jump = p[:, lanes] - f[0:RIM, lanes]
            pulled = jnp.concatenate(
                traction(
                    [jump[16 * c : 16 * (c + 1), :] for c in range(3)],
                    [zc[c : c + 1, lanes] for c in range(3)],
                    zc[3:4, lanes],
                    zc[4:5, lanes],
                ),
                axis=0,
            )
            high, low = halves(pulled)
            change = jnp.dot(
                zmat[...], jnp.concatenate([high, low, high], axis=0), preferred_element_type=F32
            )
            if last:
                f[:, lanes] = change
                continue
            v[:, lanes] = v[:, lanes] + change
            f[:, lanes] = fp[:, lanes] + DT * change
            if keep:
                ch[:, lanes] = change[0:RIM, :]

    def pair(turn, carry):
        local()
        pack(2 * turn + 1, fp)
        send(2 * turn + 1)
        receive(2 * turn, p)
        ratio[...] = p[FN : FN + 1, :] * (jac_ref[...].reshape(1, elements) * -DT)
        rim(True)
        local()
        receive(2 * turn + 1, p)
        for at in range(0, elements, 2 * LANES):
            lanes = pl.ds(at, 2 * LANES)
            p[:, lanes] = p[:, lanes] + ratio[0:1, lanes] * ch[:, lanes]
        rim(False)
        pack(2 * turn + 2, f)
        send(2 * turn + 2)
        return carry

    pl.semaphore_wait(barrier, (GROUPS - 1) * SUBS + 2)
    send(0)

    lax.fori_loop(0, ROUNDS - 1, pair, 0)
    local()
    empty(v, ovp)
    empty(fp, ofp)
    receive(2 * ROUNDS - 2, p)
    rim(False, True)
    empty(f, oc)
    for turn in range(MESSAGES):
        pltpu.make_async_copy(xs.at[turn], xs.at[turn], xs_sem.at[turn]).wait()
        for side in range(2):
            side_copy(turn, side).wait_send()


def shards(*args):
    elements = args[0].shape[2]
    shape = jax.ShapeDtypeStruct(args[0].shape, F32)
    args = args[:4] + (args[4].T,) + args[5:] + tuple(jnp.asarray(t) for t in tables())
    slots = (GROUPS - 1) * SUBS
    vmem = pl.BlockSpec(memory_space=pltpu.VMEM)
    speed, place, change = pl.pallas_call(
        kernel,
        out_shape=(pltpu.VMEM(shape.shape, F32),) * 3,
        in_specs=[pl.BlockSpec(memory_space=pl.ANY)] * len(args),
        out_specs=(vmem, vmem, vmem),
        scratch_shapes=[pltpu.VMEM(a.shape, a.dtype) for a in args]
        + [
            pltpu.VMEM((ROWS, elements), F32),
            pltpu.VMEM((ROWS, elements), F32),
            pltpu.VMEM((ROWS, elements), F32),
            pltpu.VMEM((RIM, elements), F32),
            pltpu.VMEM((RIM, elements), F32),
            pltpu.VMEM((PIECES * ROWS, 3 * ROWS), BF16),
            pltpu.VMEM((3 * RIM, 2 * ROWS), BF16),
            pltpu.VMEM((ROWS, 9 * RIM), BF16),
            pltpu.VMEM((ROWS, 3 * RIM), BF16),
            pltpu.VMEM((2 * ROWS, elements), BF16),
            pltpu.VMEM((3 * RIM, elements), F32),
            pltpu.VMEM((6 * RIM, elements), BF16),
            pltpu.VMEM((PIECES, elements), F32),
            pltpu.VMEM((1, elements), F32),
            pltpu.VMEM((3, 5, elements), F32),
            pltpu.VMEM((3, 2, elements), jnp.int32),
            pltpu.VMEM((5, elements), F32),
            pltpu.VMEM((MESSAGES, slots, LINES, LANES), F32),
            pltpu.VMEM((MESSAGES, slots, LINES, LANES), F32),
            pltpu.VMEM((MESSAGES, 2, RIM, LANES), F32),
            pltpu.VMEM((MESSAGES, 2, RIM, LANES), F32),
            pltpu.SemaphoreType.DMA((len(args),)),
            pltpu.SemaphoreType.DMA((MESSAGES,)),
            pltpu.SemaphoreType.DMA((MESSAGES,)),
            pltpu.SemaphoreType.DMA((MESSAGES, 2)),
            pltpu.SemaphoreType.DMA((MESSAGES, 2)),
        ],
        compiler_params=pltpu.CompilerParams(collective_id=0, has_side_effects=True),
    )(*args)
    return place + DT * change, speed + change


def solution(mesh):
    lanes = P(None, ("group", "sub"))
    state = P(None, None, ("group", "sub"))
    flat = P(("group", "sub"))
    return jax.shard_map(
        shards,
        mesh=mesh,
        in_specs=(state, state, lanes, flat, P(), P(), P(), lanes, lanes, lanes, lanes, flat, lanes),
        out_specs=(state, state),
        check_vma=False,
    )
```
